32 devices in a mesh: layer: 4 (over y, x), row: 2 (over core), col: 4 (over z).
Axes of the slice: x: 2, y: 2, z: 4, core: 2. Of those that a mesh axis runs over, the one named last changes fastest.
Arguments:
- block_values: bfloat16 [4, 2, 4, 32, 256, 256], P('layer', 'row', 'col'), may hold values from 0 to 3
- block_rows: int32 [4, 2, 4, 32], P('layer', 'row', 'col'), may hold values from 0 to 255
- block_cols: int32 [4, 2, 4, 32], P('layer', 'row', 'col'), may hold values from 0 to 127
- block_count: int32 [4, 2, 4], P('layer', 'row', 'col'), may hold values from 1 to 32, as said below
- dangling: int32 [4, 2, 4, 16384], P('layer', 'row', 'col'), may hold values 0 or 1
- start_ranks: float32 [4, 2, 4, 16384], P('layer', 'row', 'col'), may hold values from 0.2 to 5
Outputs:
- ranks: float32 [4, 2, 4, 16384], P('layer', 'row', 'col')
- residuals: float32 [3, 4], P(None, 'layer')
The draws below stay inside these ranges and needn't reach their ends.
Inputs may be any that keep to these rules, and one draw needn't show every extreme that they name: `block_count`: live slots of a tile; in every layer some tile has all 32 slots live. `block_rows`: slots at or past a tile's count carry no edges; coordinates may repeat within a tile, and repeated blocks add.
All inputs are finite; a program needn't handle non-finite values. No bound on the sum of `dangling` on one device may be relied on, other than what follows from the above.
Results may differ from the reference program's by a relative error of at most 0.0012.
Values may be sent and summed in bfloat16 or wider, within the bound.
A program may use at most 64 MiB of HBM per device.

```python
import math
import jax
import jax.numpy as jnp
from jax import lax

BLOCK = 256
MAXB = 32
ITERS = 3
ROW_BLK = 256
LAYERS = 4
NODES = 131072
SPAN = 16384
COL_BLK = 128
N_ROW = 2
N_COL = 4


def draw_block_values(key, part):
    shape = (LAYERS, N_ROW, N_COL, MAXB, BLOCK, BLOCK)
    first_key = jax.random.fold_in(jax.random.fold_in(key, 11), 0)
    values = jnp.exp(jax.random.uniform(first_key, shape, jnp.float32, math.log(0.05), 0.0))
    return values.astype(jnp.bfloat16)


def draw_block_count(key, part):
    first_key, second_key = jax.random.split(jax.random.fold_in(key, 23))
    tiles = N_ROW * N_COL
    counts = jax.random.randint(first_key, (LAYERS, tiles), max(1, MAXB // 4), MAXB + 1, jnp.int32)
    fullest = jax.random.randint(second_key, (LAYERS, 1), 0, tiles, jnp.int32)
    counts = jnp.where(jnp.arange(tiles, dtype=jnp.int32)[None, :] == fullest, MAXB, counts)
    return counts.reshape(LAYERS, N_ROW, N_COL).astype(jnp.int32)


def touch_ends(values, rng, low, largest):
    dims = values.shape
    index_at = [jax.random.randint(jax.random.fold_in(rng, axis), (), 0, dims[axis]) for axis in range(len(dims))]
    values = values.at[tuple(index_at)].set(low)
    longest = dims.index(max(dims))
    index_at[longest] = (index_at[longest] + 1) % dims[longest]
    return values.at[tuple(index_at)].set(largest)


def steps_of(rng, dims, cuts, smallest, largest):
    level, own = 1.0, jax.random.fold_in(rng, 6)
    for axis_at, parts in cuts:
        draws = jnp.exp(jax.random.uniform(jax.random.fold_in(own, axis_at), (parts,), jnp.float32, smallest / len(cuts), largest / len(cuts)))
        level = level * jnp.repeat(draws, dims[axis_at] // parts).reshape([-1 if axis == axis_at else 1 for axis in range(len(dims))])
    return level


def setup_inputs(seed: int = 0) -> dict:
    arg_keys = jax.random.split(jax.random.key(seed), 7)
    return {
        "block_values": draw_block_values(jax.random.fold_in(arg_keys[6], 71), 0),
        "block_rows": touch_ends(jax.random.randint(arg_keys[1], (LAYERS, N_ROW, N_COL, MAXB), 0, ROW_BLK), jax.random.fold_in(arg_keys[1], 1), 0, ROW_BLK - 1).astype(jnp.int32),
        "block_cols": touch_ends(jax.random.randint(arg_keys[2], (LAYERS, N_ROW, N_COL, MAXB), 0, COL_BLK), jax.random.fold_in(arg_keys[2], 1), 0, COL_BLK - 1).astype(jnp.int32),
        "block_count": draw_block_count(jax.random.fold_in(arg_keys[6], 71), 0),
        "dangling": touch_ends((jax.random.randint(arg_keys[4], (LAYERS, N_ROW, N_COL, SPAN), 0, 8) < 1).astype(jnp.int32), jax.random.fold_in(arg_keys[4], 1), 0, 1),
        "start_ranks": jnp.clip(jnp.exp(math.log(5.0) - 3.218876 * jax.random.uniform(arg_keys[5], (LAYERS, N_ROW, N_COL, SPAN), jnp.float32) ** steps_of(arg_keys[5], (LAYERS, N_ROW, N_COL, SPAN), ((0, 4), (1, 2), (2, 4)), -0.2, 0.2)), 0.2, 5.0),
    }


damping = 0.85
coupling = 0.3


def reference(block_values, block_rows, block_cols, block_count, dangling, start_ranks):
    live_slot = (jnp.arange(MAXB)[None, None, None, :] < block_count[..., None]).astype(jnp.float32)

    def degree_layer(packed):
        values, cols_here, live_here = packed
        colsum = jnp.einsum('rcsij->rcsj', values.astype(jnp.float32))
        onehot = (cols_here[..., None] == jnp.arange(COL_BLK)[None, None, None, :]).astype(jnp.float32) * live_here[..., None]
        deg_group = jnp.einsum('rcsb,rcsj->cbj', onehot, colsum, precision=lax.Precision.HIGHEST)
        return jnp.transpose(deg_group.reshape(N_COL, N_ROW, SPAN), (1, 0, 2))

    degree = lax.map(degree_layer, (block_values, block_cols, live_slot))
    keep_mask = 1.0 - dangling.astype(jnp.float32)
    denominator = keep_mask * degree + 1.0
    layer_ids = jnp.arange(LAYERS)
    spread = jnp.where((layer_ids == 0) | (layer_ids == LAYERS - 1), 1.0, 0.5).astype(jnp.float32) * coupling
    spread = spread.reshape(LAYERS, 1, 1, 1)

    def walk_layer(packed):
        values, rows_here, cols_here, live_here, scaled_here = packed
        column_bf = jnp.transpose(scaled_here, (1, 0, 2)).reshape(N_COL, COL_BLK, BLOCK)
        picked = column_bf[jnp.arange(N_COL)[None, :, None], cols_here]
        products = jnp.einsum('rcsij,rcsj->rcsi', values.astype(jnp.float32), picked.astype(jnp.float32))
        onehot = (rows_here[..., None] == jnp.arange(ROW_BLK)[None, None, None, :]).astype(jnp.float32) * live_here[..., None]
        walk_sum = jnp.einsum('rcsb,rcsi->rbi', onehot, products, precision=lax.Precision.HIGHEST)
        return walk_sum.reshape(N_ROW, N_COL, SPAN)

    ranks_now = start_ranks
    residual_list = []
    for iteration in range(ITERS):
        scaled = (ranks_now * keep_mask / denominator).astype(jnp.bfloat16)
        walk_sum = lax.map(walk_layer, (block_values, block_rows, block_cols, live_slot, scaled))
        dangle_mass = jnp.sum(ranks_now / denominator, axis=(1, 2, 3), keepdims=True)
        spill = ranks_now * spread
        padded = jnp.pad(spill, ((1, 1), (0, 0), (0, 0), (0, 0)))
        arrive = padded[:-2] + padded[2:]
        updated = damping * ((1.0 - coupling) * (walk_sum + dangle_mass / NODES) + arrive) + (1.0 - damping)
        residual_list.append(jnp.sum(jnp.abs(updated - ranks_now), axis=(1, 2, 3)))
        ranks_now = updated
    return ranks_now, jnp.stack(residual_list)
```

```python
import functools

import jax
import jax.numpy as jnp
from jax import lax
from jax.experimental import pallas as pl
from jax.experimental.pallas import tpu as pltpu
from jax.sharding import PartitionSpec as P

ITERS = 3
CHUNK = 16

damping = 0.85
coupling = 0.3


def fold(v):
    rows, lanes = v.shape
    acc = v[:, 0:128]
    for h in range(1, lanes // 128):
        acc = acc + v[:, h * 128 : (h + 1) * 128]
    return jnp.sum(acc.reshape(rows // 8, 8, 128), axis=0)


def split(v):
    hi = v.astype(jnp.bfloat16)
    lo = (v - hi.astype(jnp.float32)).astype(jnp.bfloat16)
    return hi, lo


def dot(a, b):
    return jnp.dot(a, b, preferred_element_type=jnp.float32)


def kernel(
    nl, nr, nc, nodes,
    values_hbm, rows_hbm, cols_hbm, count_hbm, dang_hbm, start_hbm,
    ranks_ref, resid_ref,
    values, dang_in, start_in, x_ref, inv_ref, kinv_ref,
    colsum, ohrow, ohcol, own_prod, chg,
    px_recv, pd_recv, col_send, col_recv, cs_recv, row_send, row_recv,
    sc_send, sc_recv, ma_send, ma_recv,
    pr_send, pr_recv, sp_send, sp_recv, rs_send, rs_recv,
    rows_ref, cols_ref, count_ref,
    sem_in, sem_v,
    px_ss, px_rs, pd_ss, pd_rs, col_ss, col_rs, cs_ss, cs_rs, row_ss, row_rs, sc_ss, sc_rs, ma_ss, ma_rs,
    pr_ss, pr_rs, sp_ss, sp_rs, rs_ss, rs_rs,
):
    l, r, c = (lax.axis_index(a) for a in ("layer", "row", "col"))
    slots, edge, _ = values.shape
    blocks = x_ref.shape[0]
    halves = edge // 128
    nchunk = slots // CHUNK
    f32, bf16 = jnp.float32, jnp.bfloat16

    def remote(src, dst, ss, rs, ll, rr, cc):
        return pltpu.make_async_remote_copy(
            src_ref=src, dst_ref=dst, send_sem=ss, recv_sem=rs,
            device_id=(ll, rr, cc), device_id_type=pl.DeviceIdType.MESH,
        )

    in_d = pltpu.make_async_copy(dang_hbm, dang_in, sem_in.at[0])
    in_x = pltpu.make_async_copy(start_hbm, start_in, sem_in.at[1])
    vcopies = [
        pltpu.make_async_copy(
            values_hbm.at[pl.ds(k * CHUNK, CHUNK)], values.at[pl.ds(k * CHUNK, CHUNK)], sem_v.at[k]
        )
        for k in range(nchunk)
    ]
    small = [
        pltpu.make_async_copy(src, dst, sem_in.at[2 + i])
        for i, (src, dst) in enumerate(
            [(rows_hbm, rows_ref), (cols_hbm, cols_ref), (count_hbm, count_ref)])
    ]
    in_x.start()
    in_d.start()
    for cp in small:
        cp.start()
    for cp in vcopies:
        cp.start(priority=1)

    peers = [(dr, dc) for dr in range(nr) for dc in range(nc) if (dr, dc) != (0, 0)]
    barrier = pltpu.get_barrier_semaphore()
    for dr, dc in peers:
        pl.semaphore_signal(
            barrier, inc=1,
            device_id=(l, lax.rem(r + dr, nr), lax.rem(c + dc, nc)),
            device_id_type=pl.DeviceIdType.MESH,
        )

    @pl.when(l > 0)
    def _():
        pl.semaphore_signal(
            barrier, inc=1, device_id=(l - 1, r, c), device_id_type=pl.DeviceIdType.MESH)

    @pl.when(l < nl - 1)
    def _():
        pl.semaphore_signal(
            barrier, inc=1, device_id=(l + 1, r, c), device_id_type=pl.DeviceIdType.MESH)

    for cp in small:
        cp.wait()
    live = lax.broadcasted_iota(jnp.int32, (1, slots), 1) < count_ref[...]
    rows = jnp.where(live, rows_ref[...], -1)
    cols = jnp.where(live, cols_ref[...], -1)
    row_send[...] = jnp.broadcast_to(
        jnp.concatenate([rows, jnp.full((1, 128 - slots), -1, jnp.int32)], axis=1), (8, 128)
    ).astype(f32)
    col_send[...] = jnp.broadcast_to(
        jnp.concatenate([cols, jnp.full((1, 128 - slots), -1, jnp.int32)], axis=1), (8, 128)
    ).astype(f32)

    eye = lax.broadcasted_iota(jnp.int32, (slots, slots), 0) == lax.broadcasted_iota(
        jnp.int32, (slots, slots), 1)
    colv = jnp.sum(
        jnp.where(eye, jnp.broadcast_to(cols_ref[...], (slots, slots)).astype(f32), 0.0),
        axis=1, keepdims=True,
    )
    for d in range(nr):
        base = lax.rem(r - d + nr, nr) * blocks
        at = (lax.broadcasted_iota(jnp.int32, (slots, blocks), 1) + base).astype(f32)
        ohcol[d] = jnp.where(colv == at, 1.0, 0.0).astype(bf16)

    ones = jnp.ones((CHUNK, edge), bf16)
    rid = lax.broadcasted_iota(jnp.int32, (CHUNK, edge), 0)

    def column_sum(k):
        vcopies[k].wait()
        acc = jnp.zeros((CHUNK, edge), f32)
        for s in range(CHUNK):
            acc = jnp.where(rid == s, dot(ones, values[k * CHUNK + s]), acc)
        colsum[k] = acc

    in_x.wait()
    in_d.wait()
    for h in range(halves):
        x_ref[:, h * 128 : (h + 1) * 128] = start_in[pl.ds(h, blocks, stride=halves), :]
    column_sum(0)

    order = []
    first, last = jnp.int32(0), jnp.int32(nc - 1)
    for _ in range(nc - 1):
        left = (c - first >= last - c).astype(jnp.int32)
        order.append(left * first + (1 - left) * last)
        first, last = first + left, last - (1 - left)
    far = [(cc, lax.rem(cc - c + nc, nc)) for cc in order]
    far_peers = [(dr, cc, d) for cc, d in far for dr in range(nr)]
    far_peers += [(dr, c, 0) for dr in range(1, nr)]
    sent = []

    pl.semaphore_wait(
        barrier, len(peers) + (l > 0).astype(jnp.int32) + (l < nl - 1).astype(jnp.int32))

    px, pd, pc, pcs, prow = [], [], [], [], []
    for d in range(1, nr):
        rr = lax.rem(r + d, nr)
        px.append(remote(start_in, px_recv.at[d], px_ss.at[d], px_rs.at[d], l, rr, c))
        pd.append(remote(dang_in, pd_recv.at[d], pd_ss.at[d], pd_rs.at[d], l, rr, c))
        pc.append(remote(col_send, col_recv.at[d], col_ss.at[d], col_rs.at[d], l, rr, c))
        pcs.append([
            remote(colsum.at[k], cs_recv.at[d, k], cs_ss.at[d, k], cs_rs.at[d, k], l, rr, c)
            for k in range(nchunk)
        ])
    for cc, d in far:
        prow.append(remote(row_send, row_recv.at[d], row_ss.at[d], row_rs.at[d], l, r, cc))
    for cp in px + pd + pc + prow + [q[0] for q in pcs]:
        cp.start()

    def spill_copies(t):
        return (
            remote(sp_send.at[t], sp_recv.at[t, 0], sp_ss.at[t, 0], sp_rs.at[t, 0], l + 1, r, c),
            remote(sp_send.at[t], sp_recv.at[t, 1], sp_ss.at[t, 1], sp_rs.at[t, 1], l - 1, r, c),
        )

    spread = jnp.where((l == 0) | (l == nl - 1), 1.0, 0.5).astype(f32) * coupling

    def send_spill(t, x):
        sp_send[t] = (x * spread).astype(sp_send.dtype)
        up, down = spill_copies(t)

        @pl.when(l < nl - 1)
        def _():
            up.start()

        @pl.when(l > 0)
        def _():
            down.start()

    @pl.when(l == 0)
    def _():
        for t in range(ITERS):
            sp_recv[t, 0] = jnp.zeros((blocks, edge), sp_recv.dtype)

    @pl.when(l == nl - 1)
    def _():
        for t in range(ITERS):
            sp_recv[t, 1] = jnp.zeros((blocks, edge), sp_recv.dtype)

    send_spill(0, x_ref[...])

    for k in range(1, nchunk):
        column_sum(k)
        for q in pcs:
            q[k].start()

    def spread_sums(tab, sums, rr):
        at = (lax.broadcasted_iota(jnp.int32, (blocks, slots), 0) + rr * blocks).astype(f32)
        oh = jnp.where(
            jnp.broadcast_to(tab[0:1, 0:slots], (blocks, slots)) == at, 1.0, 0.0).astype(bf16)
        hi, lo = split(sums.reshape(slots, edge))
        return dot(oh, hi) + dot(oh, lo)

    def piece(buf, h):
        return buf[pl.ds(h, blocks, stride=halves), :]

    near = [spread_sums(col_send, colsum[...], lax.rem(r - d + nr, nr)) for d in range(nr)]
    for cp in px + pd + pc:
        cp.wait_recv()
    peer_x = {d: jnp.concatenate([piece(px_recv.at[d], h) for h in range(halves)], axis=1)
              for d in range(1, nr)}
    keeps = {d: 1.0 - jnp.concatenate(
        [piece(pd_recv.at[d] if d else dang_in, h) for h in range(halves)], axis=1).astype(f32)
        for d in range(nr)}
    for q in pcs:
        for cp in q:
            cp.wait_recv()
    for d in range(nr):
        deg = near[d]
        for e in range(1, nr):
            deg = deg + spread_sums(col_recv[e], cs_recv[e], lax.rem(r - d + nr, nr))
        inv = 1.0 / (keeps[d] * deg + 1.0)
        kinv = keeps[d] * inv
        if d == 0:
            inv_ref[...] = inv
            kinv_ref[...] = kinv
        else:
            sc_recv[0, d] = (peer_x[d] * kinv).astype(bf16)

    def row_onehot(tab):
        at = (lax.broadcasted_iota(jnp.int32, (blocks, slots), 0) + c * blocks).astype(f32)
        return jnp.where(jnp.broadcast_to(tab[0:1, 0:slots], (blocks, slots)) == at,
                         1.0, 0.0).astype(bf16)

    def step(t):
        x = x_ref[...]
        scaled = (x * kinv_ref[...]).astype(bf16)
        if t > 0:
            sc_send[t] = scaled
        sc = [
            remote(sc_send.at[t], sc_recv.at[t, d], sc_ss.at[t, d], sc_rs.at[t, d],
                   l, lax.rem(r + d, nr), c)
            for d in range(1, nr)
            if t > 0
        ]
        for cp in sc:
            cp.start()
        mass_own = jnp.sum(fold(x * inv_ref[...]), axis=0, keepdims=True)
        ma_send[t] = mass_own
        ma = []
        for i, (dr, cc, dc) in enumerate(far_peers):
            slot = dr * nc + dc - 1
            ma.append(remote(ma_send.at[t], ma_recv.at[t, slot], ma_ss.at[t, slot],
                             ma_rs.at[t, slot], l, lax.rem(r + dr, nr), cc))
        for cp in ma:
            cp.start()

        if t > 0:
            send_spill(t, x)

        picked = dot(ohcol[0], scaled)
        for d in range(1, nr):
            if t > 0:
                sc[d - 1].wait_recv()
            picked = picked + dot(ohcol[d], sc_recv[t, d])
        picked = picked.astype(bf16)

        pr = []
        for k in range(nchunk):
            lhs = picked[k * CHUNK : (k + 1) * CHUNK]
            acc = jnp.zeros((CHUNK, edge), f32)
            for s in range(CHUNK):
                res = lax.dot_general(
                    lhs, values[k * CHUNK + s], (((1,), (1,)), ((), ())),
                    preferred_element_type=f32)
                acc = jnp.where(rid == s, res, acc)
            own_prod[k * CHUNK : (k + 1) * CHUNK] = acc
            pr_send[t, k] = acc.astype(pr_send.dtype)
            for cc, d in far:
                cp = remote(pr_send.at[t, k], pr_recv.at[t, d, k], pr_ss.at[t, d, k],
                            pr_rs.at[t, d, k], l, r, cc)
                cp.start()
                pr.append(cp)

        if t == 0:
            ohrow[0] = row_onehot(row_send)
            for cp in prow:
                cp.wait_recv()
            for d in range(1, nc):
                ohrow[d] = row_onehot(row_recv[d])

        phi, plo = split(own_prod[...])
        walk = dot(ohrow[0], phi) + dot(ohrow[0], plo)

        up, down = spill_copies(t)

        @pl.when(l > 0)
        def _():
            up.wait_recv()

        @pl.when(l < nl - 1)
        def _():
            down.wait_recv()

        arrive = sp_recv[t, 0].astype(f32) + sp_recv[t, 1].astype(f32)
        mass = mass_own
        for cp in ma:
            cp.wait_recv()
        for i in range(len(peers)):
            mass = mass + ma_recv[t, i]
        rest = damping * ((1.0 - coupling) * (jnp.sum(mass) / nodes) + arrive) + (1.0 - damping)

        for d in range(1, nc):
            for k in range(nchunk):
                remote(pr_send.at[t, k], pr_recv.at[t, d, k], pr_ss.at[t, d, k], pr_rs.at[t, d, k], l, r, lax.rem(c + d, nc)).wait_recv()
            got = pr_recv[t, d].reshape(slots, edge)
            if got.dtype == bf16:
                walk = walk + dot(ohrow[d], got)
            else:
                ghi, glo = split(got)
                walk = walk + dot(ohrow[d], ghi) + dot(ohrow[d], glo)
        updated = damping * (1.0 - coupling) * walk + rest
        x_ref[...] = updated
        chg[t] = fold(jnp.abs(updated - x))

        sent.extend(sc + ma + pr)

    for t in range(ITERS):
        step(t)

    lane = lax.broadcasted_iota(jnp.int32, (1, 128), 1)
    changes = jnp.zeros((1, 128), f32)
    for t in range(ITERS):
        changes = jnp.where(lane == t, jnp.sum(chg[t]), changes)
    rs_send[...] = changes
    rs = []
    for dr, cc, dc in far_peers:
        i = dr * nc + dc - 1
        cp = remote(rs_send, rs_recv.at[i], rs_ss.at[i], rs_rs.at[i],
                    l, lax.rem(r + dr, nr), cc)
        cp.start()
        rs.append(cp)
    for h in range(halves):
        ranks_ref[pl.ds(h, blocks, stride=halves), :] = x_ref[:, h * 128 : (h + 1) * 128]
    for cp in px + pd + pc + prow + [e for q in pcs for e in q] + sent:
        cp.wait_send()
    ups = [spill_copies(t) for t in range(ITERS)]

    @pl.when(l < nl - 1)
    def _():
        for up, _ in ups:
            up.wait_send()

    @pl.when(l > 0)
    def _():
        for _, down in ups:
            down.wait_send()

    total = rs_send[...]
    for cp in rs:
        cp.wait_recv()
    for i in range(len(peers)):
        total = total + rs_recv[i]
    resid_ref[...] = total
    for cp in rs:
        cp.wait_send()


def scoped(sems, *args):
    pl.run_scoped(lambda *refs: kernel(*args, *refs), *sems)


def finish(ranks_in, resid_in, ranks_ref, resid_ref):
    ranks_ref[...] = ranks_in[...]
    resid_ref[...] = resid_in[:, 0:ITERS]


def local(block_values, block_rows, block_cols, block_count, dangling, start_ranks):
    span = start_ranks.shape[-1]
    nl, nr, nc = (lax.axis_size(a) for a in ("layer", "row", "col"))
    slots, edge = block_values.shape[3], block_values.shape[-1]
    blocks = span // edge
    nchunk = slots // CHUNK
    nodes = nr * nc * span
    npeer = nr * nc - 1
    f32, bf16 = jnp.float32, jnp.bfloat16
    vm, dma = pltpu.VMEM, pltpu.SemaphoreType.DMA
    big = (blocks, edge)
    PT, ST = bf16, bf16
    scratch = [
        vm((slots, edge, edge), bf16), vm((span // 128, 128), jnp.int32), vm((span // 128, 128), f32),
        vm(big, f32), vm(big, f32), vm(big, f32),
        vm((nchunk, CHUNK, edge), f32), vm((nc, blocks, slots), bf16), vm((nr, slots, blocks), bf16),
        vm((slots, edge), f32), vm((ITERS, 8, 128), f32),
        vm((nr, span // 128, 128), f32), vm((nr, span // 128, 128), jnp.int32),
        vm((8, 128), f32), vm((nr, 8, 128), f32), vm((nr, nchunk, CHUNK, edge), f32),
        vm((8, 128), f32), vm((nc, 8, 128), f32),
        vm((ITERS,) + big, bf16), vm((ITERS, nr) + big, bf16),
        vm((ITERS, 1, 128), f32), vm((ITERS, npeer, 1, 128), f32),
        vm((ITERS, nchunk, CHUNK, edge), PT), vm((ITERS, nc, nchunk, CHUNK, edge), PT),
        vm((ITERS,) + big, ST), vm((ITERS, 2) + big, ST),
        vm((1, 128), f32), vm((npeer, 1, 128), f32),
        vm((1, slots), jnp.int32), vm((1, slots), jnp.int32), vm((1, 1), jnp.int32),
    ]
    sems = [
        dma((5,)), dma((nchunk,)),
        dma((nr,)), dma((nr,)), dma((nr,)), dma((nr,)), dma((nr,)), dma((nr,)),
        dma((nr, nchunk)), dma((nr, nchunk)), dma((nc,)), dma((nc,)),
        dma((ITERS, nr)), dma((ITERS, nr)), dma((ITERS, npeer)), dma((ITERS, npeer)),
        dma((ITERS, nc, nchunk)), dma((ITERS, nc, nchunk)),
        dma((ITERS, 2)), dma((ITERS, 2)), dma((npeer,)), dma((npeer,)),
    ]
    hbm = pl.BlockSpec(memory_space=pltpu.HBM)
    vmem = pl.BlockSpec(memory_space=pltpu.VMEM)
    ranks, resid = pl.pallas_call(
        functools.partial(scoped, sems, nl, nr, nc, nodes),
        out_shape=(
            pltpu.VMEM((span // 128, 128), f32),
            pltpu.VMEM((1, 128), f32),
        ),
        in_specs=[hbm] * 6,
        out_specs=(vmem, vmem),
        scratch_shapes=scratch,
        compiler_params=pltpu.CompilerParams(collective_id=0, has_side_effects=True),
    )(
        block_values.reshape(slots, edge, edge),
        block_rows.reshape(1, slots),
        block_cols.reshape(1, slots),
        block_count.reshape(1, 1),
        dangling.reshape(span // 128, 128),
        start_ranks.reshape(span // 128, 128),
    )
    ranks, resid = pl.pallas_call(
        finish,
        out_shape=(
            jax.ShapeDtypeStruct((span // 128, 128), f32),
            jax.ShapeDtypeStruct((1, ITERS), f32),
        ),
        in_specs=[vmem, vmem],
        out_specs=(vmem, vmem),
        compiler_params=pltpu.CompilerParams(vmem_limit_bytes=4 * 1024 * 1024),
    )(ranks, resid)
    return ranks.reshape(1, 1, 1, span), resid.T


def solution(mesh):
    placed = (
        P("layer", "row", "col", None, None, None),
        P("layer", "row", "col", None),
        P("layer", "row", "col", None),
        P("layer", "row", "col"),
        P("layer", "row", "col", None),
        P("layer", "row", "col", None),
    )
    return jax.shard_map(
        local,
        mesh=mesh,
        in_specs=placed,
        out_specs=(P("layer", "row", "col", None), P(None, "layer")),
        check_vma=False,
    )
```

```python
import functools

import jax
import jax.numpy as jnp
from jax import lax
from jax.experimental import pallas as pl
from jax.experimental.pallas import tpu as pltpu
from jax.sharding import PartitionSpec as P

ITERS = 3
CHUNK = 16
PIECE = 8
CUTS = (16, 16)

damping = 0.85
coupling = 0.3


def fold(v):
    rows, lanes = v.shape
    acc = v[:, 0:128]
    for h in range(1, lanes // 128):
        acc = acc + v[:, h * 128 : (h + 1) * 128]
    return jnp.sum(acc.reshape(rows // 8, 8, 128), axis=0)


def split(v):
    hi = v.astype(jnp.bfloat16)
    lo = (v - hi.astype(jnp.float32)).astype(jnp.bfloat16)
    return hi, lo


def dot(a, b):
    return jnp.dot(a, b, preferred_element_type=jnp.float32)


def kernel(
    nl, nr, nc, nodes,
    values_hbm, rows_hbm, cols_hbm, count_hbm, dang_hbm, start_hbm,
    ranks_ref, resid_ref,
    values, vt, dang_in, start_in, x_ref, inv_ref, kinv_ref,
    colsum, ohcol, own_prod, chg,
    pk_own, pk_send, pk_recv, kg_ref, hot_own, hot_far, ohq,
    px_recv, pd_recv, col_send, col_recv, cs_recv, row_send, row_recv,
    sc_recv, ma_send, ma_recv,
    pr_send, pr_recv, sp_send, sp_recv, rs_send, rs_recv,
    rows_ref, cols_ref, count_ref,
    sem_in, sem_v,
    px_ss, px_rs, pd_ss, pd_rs, col_ss, col_rs, cs_ss, cs_rs, row_ss, row_rs, sc_ss, sc_rs, ma_ss, ma_rs,
    pr_ss, pr_rs, sp_ss, sp_rs, rs_ss, rs_rs,
):
    l, r, c = (lax.axis_index(a) for a in ("layer", "row", "col"))
    slots, edge, _ = values.shape
    blocks = x_ref.shape[0]
    halves = edge // 128
    nchunk = slots // PIECE
    early = nchunk // 2
    cuts = [(sum(CUTS[:i]), n) for i, n in enumerate(CUTS)]
    f32, bf16 = jnp.float32, jnp.bfloat16

    def remote(src, dst, ss, rs, ll, rr, cc):
        return pltpu.make_async_remote_copy(
            src_ref=src, dst_ref=dst, send_sem=ss, recv_sem=rs,
            device_id=(ll, rr, cc), device_id_type=pl.DeviceIdType.MESH,
        )

    in_d = pltpu.make_async_copy(dang_hbm, dang_in, sem_in.at[0])
    in_x = pltpu.make_async_copy(start_hbm, start_in, sem_in.at[1])
    vcopies = [
        pltpu.make_async_copy(
            values_hbm.at[pl.ds(k * PIECE, PIECE)], values.at[pl.ds(k * PIECE, PIECE)], sem_v.at[k]
        )
        for k in range(nchunk)
    ]
    small = [
        pltpu.make_async_copy(src, dst, sem_in.at[2 + i])
        for i, (src, dst) in enumerate(
            [(rows_hbm, rows_ref), (cols_hbm, cols_ref), (count_hbm, count_ref)])
    ]
    in_x.start()
    in_d.start()
    for cp in small:
        cp.start()
    for cp in vcopies:
        cp.start(priority=1)

    peers = [(dr, dc) for dr in range(nr) for dc in range(nc) if (dr, dc) != (0, 0)]
    barrier = pltpu.get_barrier_semaphore()
    for dr, dc in peers:
        pl.semaphore_signal(
            barrier, inc=1,
            device_id=(l, lax.rem(r + dr, nr), lax.rem(c + dc, nc)),
            device_id_type=pl.DeviceIdType.MESH,
        )

    @pl.when(l > 0)
    def _():
        pl.semaphore_signal(
            barrier, inc=1, device_id=(l - 1, r, c), device_id_type=pl.DeviceIdType.MESH)

    @pl.when(l < nl - 1)
    def _():
        pl.semaphore_signal(
            barrier, inc=1, device_id=(l + 1, r, c), device_id_type=pl.DeviceIdType.MESH)

    for cp in small:
        cp.wait()
    live = lax.broadcasted_iota(jnp.int32, (1, slots), 1) < count_ref[...]
    rows = jnp.where(live, rows_ref[...], -1)
    cols = jnp.where(live, cols_ref[...], -1)
    row_send[...] = jnp.broadcast_to(
        jnp.concatenate([rows, jnp.full((1, 128 - slots), -1, jnp.int32)], axis=1), (8, 128)
    ).astype(f32)
    col_send[...] = jnp.broadcast_to(
        jnp.concatenate([cols, jnp.full((1, 128 - slots), -1, jnp.int32)], axis=1), (8, 128)
    ).astype(f32)

    eye = lax.broadcasted_iota(jnp.int32, (slots, slots), 0) == lax.broadcasted_iota(
        jnp.int32, (slots, slots), 1)

    def upright(tab):
        return jnp.sum(
            jnp.where(eye, jnp.broadcast_to(tab, (slots, slots)), 0.0), axis=1, keepdims=True)

    colv = upright(cols_ref[...].astype(f32))
    for d in range(nr):
        base = lax.rem(r - d + nr, nr) * blocks
        at = (lax.broadcasted_iota(jnp.int32, (slots, blocks), 1) + base).astype(f32)
        ohcol[d] = jnp.where(colv == at, 1.0, 0.0).astype(bf16)

    ones = jnp.ones((CHUNK, edge), bf16)
    rid = lax.broadcasted_iota(jnp.int32, (PIECE, edge), 0)

    def column_sum(k):
        vcopies[k].wait()
        acc = jnp.zeros((PIECE, edge), f32)
        for s in range(PIECE):
            acc = jnp.where(rid == s, dot(ones, values[k * PIECE + s])[0:PIECE], acc)
        colsum[k] = acc

    def transpose(k):
        for s in range(k * PIECE, (k + 1) * PIECE):
            vt[s] = values[s].T

    in_x.wait()
    in_d.wait()
    for h in range(halves):
        x_ref[:, h * 128 : (h + 1) * 128] = start_in[pl.ds(h, blocks, stride=halves), :]
    column_sum(0)

    order = []
    first, last = jnp.int32(0), jnp.int32(nc - 1)
    for _ in range(nc - 1):
        left = (c - first >= last - c).astype(jnp.int32)
        order.append(left * first + (1 - left) * last)
        first, last = first + left, last - (1 - left)
    far = [(cc, lax.rem(cc - c + nc, nc)) for cc in order]
    far_peers = [(dr, cc, d) for cc, d in far for dr in range(nr)]
    far_peers += [(dr, c, 0) for dr in range(1, nr)]
    sent = []

    for k in range(1, nchunk - 1):
        column_sum(k)

    pl.semaphore_wait(
        barrier, len(peers) + (l > 0).astype(jnp.int32) + (l < nl - 1).astype(jnp.int32))

    px, pd, pc, pcs, prow = [], [], [], [], []
    for d in range(1, nr):
        rr = lax.rem(r + d, nr)
        px.append(remote(start_in, px_recv.at[d], px_ss.at[d], px_rs.at[d], l, rr, c))
        pd.append(remote(dang_in, pd_recv.at[d], pd_ss.at[d], pd_rs.at[d], l, rr, c))
        pc.append(remote(col_send, col_recv.at[d], col_ss.at[d], col_rs.at[d], l, rr, c))
        pcs.append([
            remote(colsum.at[k], cs_recv.at[d, k], cs_ss.at[d, k], cs_rs.at[d, k], l, rr, c)
            for k in range(nchunk)
        ])
    for cc, d in far:
        prow.append(remote(row_send, row_recv.at[d], row_ss.at[d], row_rs.at[d], l, r, cc))
    for cp in [cp for q in pcs for cp in q[:-1]] + px + pd + pc:
        cp.start()

    def spill_copies(t):
        return (
            remote(sp_send.at[t], sp_recv.at[t, 0], sp_ss.at[t, 0], sp_rs.at[t, 0], l + 1, r, c),
            remote(sp_send.at[t], sp_recv.at[t, 1], sp_ss.at[t, 1], sp_rs.at[t, 1], l - 1, r, c),
        )

    spread = jnp.where((l == 0) | (l == nl - 1), 1.0, 0.5).astype(f32) * coupling

    def send_spill(t, x, when):
        if x is not None:
            sp_send[t] = (x * spread).astype(sp_send.dtype)
        up, down = spill_copies(t)

        @pl.when((l < nl - 1) & when)
        def _():
            up.start()

        @pl.when((l > 0) & when)
        def _():
            down.start()

    @pl.when(l == 0)
    def _():
        for t in range(ITERS):
            sp_recv[t, 0] = jnp.zeros((blocks, edge), sp_recv.dtype)

    @pl.when(l == nl - 1)
    def _():
        for t in range(ITERS):
            sp_recv[t, 1] = jnp.zeros((blocks, edge), sp_recv.dtype)

    column_sum(nchunk - 1)
    for q in pcs:
        q[-1].start()
    for k in range(early):
        transpose(k)

    def hot(tab, rr):
        at = (lax.broadcasted_iota(jnp.int32, (blocks, slots), 0) + rr * blocks).astype(f32)
        return jnp.where(
            jnp.broadcast_to(tab[0:1, 0:slots], (blocks, slots)) == at, 1.0, 0.0).astype(bf16)

    def spread_sums(oh, sums):
        hi, lo = split(sums.reshape(slots, edge))
        return dot(oh, hi) + dot(oh, lo)

    def piece(buf, h):
        return buf[pl.ds(h, blocks, stride=halves), :]

    whose = [lax.rem(r - d + nr, nr) for d in range(nr)]
    near = [spread_sums(hot(col_send, rr), colsum[...]) for rr in whose]
    for cp in px + pd + pc:
        cp.wait_recv()
    peer_x = {d: jnp.concatenate([piece(px_recv.at[d], h) for h in range(halves)], axis=1)
              for d in range(1, nr)}
    keeps = {d: 1.0 - jnp.concatenate(
        [piece(pd_recv.at[d] if d else dang_in, h) for h in range(halves)], axis=1).astype(f32)
        for d in range(nr)}
    hots = [[hot(col_recv[e], rr) for e in range(1, nr)] for rr in whose]
    for e in range(nr):
        tab = colv if e == 0 else upright(col_recv[e][0:1, 0:slots])
        at = (lax.broadcasted_iota(jnp.int32, (slots, blocks), 1) + r * blocks).astype(f32)
        ohq[e * slots : (e + 1) * slots] = jnp.where(tab == at, 1.0, 0.0).astype(bf16)
    for q in pcs:
        for cp in q:
            cp.wait_recv()
    for cp in prow:
        cp.start()
    send_spill(0, x_ref[...], r >= 0)
    for d in range(nr):
        deg = near[d]
        for e in range(1, nr):
            deg = deg + spread_sums(hots[d][e - 1], cs_recv[e])
        inv = 1.0 / (keeps[d] * deg + 1.0)
        kinv = keeps[d] * inv
        if d == 0:
            inv_ref[...] = inv
            kinv_ref[...] = kinv
        else:
            sc_recv[d] = (peer_x[d] * kinv).astype(bf16)

    def row_onehot(tabs):
        tab = jnp.concatenate([tab[0:1, 0:slots] for tab in tabs], axis=1)
        shape = (blocks, tab.shape[1])
        at = (lax.broadcasted_iota(jnp.int32, shape, 0) + c * blocks).astype(f32)
        return jnp.where(jnp.broadcast_to(tab, shape) == at, 1.0, 0.0).astype(bf16)

    def pick_copies(t):
        return [
            remote(pk_send.at[t, d], pk_recv.at[t, d], sc_ss.at[t, d], sc_rs.at[t, d],
                   l, lax.rem(r + d, nr), c)
            for d in range(1, nr)
        ]

    def picks(t):
        if t == 0:
            acc = dot(ohcol[0], (x_ref[...] * kinv_ref[...]).astype(bf16))
            for d in range(1, nr):
                acc = acc + dot(ohcol[d], sc_recv[d])
            return acc.astype(bf16)
        acc = pk_own[...]
        for d, cp in enumerate(pick_copies(t), 1):
            cp.wait_recv()
            acc = acc + pk_recv[t, d].astype(f32)
        return acc.astype(bf16)

    def products(t):
        picked = picks(t)
        if t > 0:
            send_spill(t, None, lax.rem(r, 2) == 0)
        def piece_copy(k, cc, d):
            at, n = cuts[k]
            return remote(
                pr_send.at[t, pl.ds(at, n)], pr_recv.at[t, d, pl.ds(at, n)], pr_ss.at[t, d, k],
                pr_rs.at[t, d, k], l, r, cc)

        pr = []
        for k, (at, n) in enumerate(cuts):
            for at in range(at, at + n, PIECE):
                base = at // CHUNK * CHUNK
                lhs = picked[base : base + CHUNK]
                acc = jnp.zeros((PIECE, edge), f32)
                for s in range(PIECE):
                    if t == 0 and at >= early * PIECE:
                        res = lax.dot_general(
                            lhs, values[at + s], (((1,), (1,)), ((), ())),
                            preferred_element_type=f32)
                    else:
                        res = dot(lhs, vt[at + s])
                    acc = jnp.where(rid == s, res[at - base : at - base + PIECE], acc)
                own_prod[at : at + PIECE] = acc
                pr_send[t, at : at + PIECE] = acc.astype(pr_send.dtype)
            pr += [piece_copy(k, *to) for to in (far[:-1] if k < len(cuts) - 1 else far)]
            for cp in pr[-len(far) + (k < len(cuts) - 1) :]:
                cp.start()
        for k in range(len(cuts) - 1):
            pr.append(piece_copy(k, *far[-1]))
            pr[-1].start()
        sent.extend(pr)

    def masses(t):
        mass_own = jnp.sum(fold(x_ref[...] * inv_ref[...]), axis=0, keepdims=True)
        ma_send[t] = mass_own
        ma = []
        for i, (dr, cc, dc) in enumerate(far_peers):
            slot = dr * nc + dc - 1
            ma.append(remote(ma_send.at[t], ma_recv.at[t, slot], ma_ss.at[t, slot],
                             ma_rs.at[t, slot], l, lax.rem(r + dr, nr), cc))
        for cp in ma:
            cp.start()
        sent.extend(ma)
        return mass_own, ma

    def note_change(t, diff):
        part = jnp.sum(fold(jnp.abs(diff)), axis=0, keepdims=True)
        lane = lax.broadcasted_iota(jnp.int32, (1, 128), 1)
        old = chg[...] if t else jnp.zeros((1, 128), f32)
        chg[...] = jnp.where(lane == t, jnp.sum(part, axis=1, keepdims=True), old)

    def step(t, mass_own, ma):
        products(t)
        if t == 0:
            for k in range(early, nchunk):
                transpose(k)
            for cp in prow:
                cp.wait_recv()
            for part, tabs in enumerate([[row_send], [row_recv.at[d] for d in range(1, nc)]]):
                oh = row_onehot(tabs)
                ref = hot_far if part else hot_own
                ref[nr * slots :] = oh
                ref[0 : nr * slots] = dot(ohq[...], oh).astype(bf16)
            khi, klo = split(kinv_ref[...])
            kg_ref[...] = dot(ohq[...], khi) + dot(ohq[...], klo)

        phi, plo = split(own_prod[...])
        last = t == ITERS - 1
        npick = 0 if last else nr * slots
        skip = nr * slots - npick
        near_sum = dot(hot_own[skip:], phi) + dot(hot_own[skip:], plo)

        up, down = spill_copies(t)

        @pl.when(l > 0)
        def _():
            up.wait_recv()

        @pl.when(l < nl - 1)
        def _():
            down.wait_recv()

        arrive = sp_recv[t, 0].astype(f32) + sp_recv[t, 1].astype(f32)
        mass = mass_own
        for cp in ma:
            cp.wait_recv()
        for i in range(len(peers)):
            mass = mass + ma_recv[t, i]
        flat = damping * (1.0 - coupling) * (jnp.sum(mass) / nodes) + (1.0 - damping)
        rest = damping * arrive + flat
        if not last:
            restg = damping * (dot(ohq[...], sp_recv[t, 0]) + dot(ohq[...], sp_recv[t, 1])) + flat

        gain = damping * (1.0 - coupling)
        if not last:
            near_pick = gain * near_sum[0:npick] + restg
        near_walk = gain * near_sum[npick:] + rest
        for d in range(1, nc):
            for k, (at, n) in enumerate(cuts):
                remote(pr_send.at[t, pl.ds(at, n)], pr_recv.at[t, d, pl.ds(at, n)],
                       pr_ss.at[t, d, k], pr_rs.at[t, d, k],
                       l, r, lax.rem(c + d, nc)).wait_recv()
        far_sum = dot(hot_far[skip:], pr_recv[t, 1:nc].reshape((nc - 1) * slots, edge))
        if not last:
            pk = kg_ref[...] * (gain * far_sum[0:npick] + near_pick)
            for d in range(1, nr):
                pk_send[t + 1, d] = pk[d * slots : (d + 1) * slots].astype(bf16)
            pk_own[...] = pk[0:slots].astype(bf16).astype(f32)
            cps = pick_copies(t + 1)
            for cp in cps:
                cp.start()
            sent.extend(cps)
        x = x_ref[...]
        updated = gain * far_sum[npick:] + near_walk
        x_ref[...] = updated
        if last:
            note_change(t, updated - x)
            return None
        send_spill(t + 1, updated, lax.rem(r, 2) == 1)
        out = masses(t + 1)
        note_change(t, updated - x)
        return out

    carry = masses(0)
    for t in range(ITERS):
        carry = step(t, *carry)

    rs_send[...] = chg[...]
    rs = []
    for dr, cc, dc in far_peers:
        i = dr * nc + dc - 1
        cp = remote(rs_send, rs_recv.at[i], rs_ss.at[i], rs_rs.at[i],
                    l, lax.rem(r + dr, nr), cc)
        cp.start()
        rs.append(cp)
    for h in range(halves):
        ranks_ref[pl.ds(h, blocks, stride=halves), :] = x_ref[:, h * 128 : (h + 1) * 128]
    for cp in px + pd + pc + prow + [e for q in pcs for e in q] + sent:
        cp.wait_send()
    ups = [spill_copies(t) for t in range(ITERS)]

    @pl.when(l < nl - 1)
    def _():
        for up, _ in ups:
            up.wait_send()

    @pl.when(l > 0)
    def _():
        for _, down in ups:
            down.wait_send()

    total = rs_send[...]
    for cp in rs:
        cp.wait_recv()
    for i in range(len(peers)):
        total = total + rs_recv[i]
    resid_ref[...] = total
    for cp in rs:
        cp.wait_send()


def scoped(sems, *args):
    pl.run_scoped(lambda *refs: kernel(*args, *refs), *sems)


def finish(ranks_in, resid_in, ranks_ref, resid_ref):
    ranks_ref[...] = ranks_in[...]
    resid_ref[...] = resid_in[:, 0:ITERS]


def local(block_values, block_rows, block_cols, block_count, dangling, start_ranks):
    span = start_ranks.shape[-1]
    nl, nr, nc = (lax.axis_size(a) for a in ("layer", "row", "col"))
    slots, edge = block_values.shape[3], block_values.shape[-1]
    blocks = span // edge
    nchunk = slots // PIECE
    nodes = nr * nc * span
    npeer = nr * nc - 1
    f32, bf16 = jnp.float32, jnp.bfloat16
    vm, dma = pltpu.VMEM, pltpu.SemaphoreType.DMA
    big = (blocks, edge)
    PT, ST = bf16, bf16
    scratch = [
        vm((slots, edge, edge), bf16), vm((slots, edge, edge), bf16), vm((span // 128, 128), jnp.int32), vm((span // 128, 128), f32),
        vm(big, f32), vm(big, f32), vm(big, f32),
        vm((nchunk, PIECE, edge), f32), vm((nr, slots, blocks), bf16),
        vm((slots, edge), f32), vm((1, 128), f32),
        vm((slots, edge), f32), vm((ITERS, nr, slots, edge), bf16), vm((ITERS, nr, slots, edge), bf16),
        vm((nr * slots, edge), f32), vm((nr * slots + blocks, slots), bf16),
        vm((nr * slots + blocks, (nc - 1) * slots), bf16), vm((nr * slots, blocks), bf16),
        vm((nr, span // 128, 128), f32), vm((nr, span // 128, 128), jnp.int32),
        vm((8, 128), f32), vm((nr, 8, 128), f32), vm((nr, nchunk, PIECE, edge), f32),
        vm((8, 128), f32), vm((nc, 8, 128), f32),
        vm((nr,) + big, bf16),
        vm((ITERS, 1, 128), f32), vm((ITERS, npeer, 1, 128), f32),
        vm((ITERS, slots, edge), PT), vm((ITERS, nc, slots, edge), PT),
        vm((ITERS,) + big, ST), vm((ITERS, 2) + big, ST),
        vm((1, 128), f32), vm((npeer, 1, 128), f32),
        vm((1, slots), jnp.int32), vm((1, slots), jnp.int32), vm((1, 1), jnp.int32),
    ]
    sems = [
        dma((5,)), dma((nchunk,)),
        dma((nr,)), dma((nr,)), dma((nr,)), dma((nr,)), dma((nr,)), dma((nr,)),
        dma((nr, nchunk)), dma((nr, nchunk)), dma((nc,)), dma((nc,)),
        dma((ITERS, nr)), dma((ITERS, nr)), dma((ITERS, npeer)), dma((ITERS, npeer)),
        dma((ITERS, nc, len(CUTS))), dma((ITERS, nc, len(CUTS))),
        dma((ITERS, 2)), dma((ITERS, 2)), dma((npeer,)), dma((npeer,)),
    ]
    hbm = pl.BlockSpec(memory_space=pltpu.HBM)
    vmem = pl.BlockSpec(memory_space=pltpu.VMEM)
    ranks, resid = pl.pallas_call(
        functools.partial(scoped, sems, nl, nr, nc, nodes),
        out_shape=(
            pltpu.VMEM((span // 128, 128), f32),
            pltpu.VMEM((1, 128), f32),
        ),
        in_specs=[hbm] * 6,
        out_specs=(vmem, vmem),
        scratch_shapes=scratch,
        compiler_params=pltpu.CompilerParams(collective_id=0, has_side_effects=True),
    )(
        block_values.reshape(slots, edge, edge),
        block_rows.reshape(1, slots),
        block_cols.reshape(1, slots),
        block_count.reshape(1, 1),
        dangling.reshape(span // 128, 128),
        start_ranks.reshape(span // 128, 128),
    )
    ranks, resid = pl.pallas_call(
        finish,
        out_shape=(
            jax.ShapeDtypeStruct((span // 128, 128), f32),
            jax.ShapeDtypeStruct((1, ITERS), f32),
        ),
        in_specs=[vmem, vmem],
        out_specs=(vmem, vmem),
        compiler_params=pltpu.CompilerParams(vmem_limit_bytes=4 * 1024 * 1024),
    )(ranks, resid)
    return ranks.reshape(1, 1, 1, span), resid.T


def solution(mesh):
    placed = (
        P("layer", "row", "col", None, None, None),
        P("layer", "row", "col", None),
        P("layer", "row", "col", None),
        P("layer", "row", "col"),
        P("layer", "row", "col", None),
        P("layer", "row", "col", None),
    )
    return jax.shard_map(
        local,
        mesh=mesh,
        in_specs=placed,
        out_specs=(P("layer", "row", "col", None), P(None, "layer")),
        check_vma=False,
    )
```

```python
import functools

import jax
import jax.numpy as jnp
from jax import lax
from jax.experimental import pallas as pl
from jax.experimental.pallas import tpu as pltpu
from jax.sharding import PartitionSpec as P

ITERS = 3
CHUNK = 16
PIECE = 8
CUTS = (16, 16)

damping = 0.85
coupling = 0.3


def fold(v):
    rows, lanes = v.shape
    acc = v[:, 0:128]
    for h in range(1, lanes // 128):
        acc = acc + v[:, h * 128 : (h + 1) * 128]
    return jnp.sum(acc.reshape(rows // 8, 8, 128), axis=0)


def split(v):
    hi = v.astype(jnp.bfloat16)
    lo = (v - hi.astype(jnp.float32)).astype(jnp.bfloat16)
    return hi, lo


def dot(a, b):
    return jnp.dot(a, b, preferred_element_type=jnp.float32)


def kernel(
    nl, nr, nc, nodes,
    values_hbm, rows_hbm, cols_hbm, count_hbm, dang_hbm, start_hbm,
    ranks_ref, resid_ref,
    values, vt, dang_in, start_in, x_ref, inv_ref, kinv_ref,
    colsum, ohcol, own_prod, diff, chg,
    pk_own, pk_send, pk_recv, kg_ref, hot_own, hot_far, ohq,
    px_recv, pd_recv, col_send, col_recv, cs_recv, row_send, row_recv,
    sc_recv, ma_send, ma_recv,
    pr_send, pr_recv, sp_send, sp_recv, rs_send, rs_recv,
    rows_ref, cols_ref, count_ref,
    sem_in, sem_v,
    px_ss, px_rs, pd_ss, pd_rs, col_ss, col_rs, cs_ss, cs_rs, row_ss, row_rs, sc_ss, sc_rs, ma_ss, ma_rs,
    ready,
    pr_ss, pr_rs, sp_ss, sp_rs, rs_ss, rs_rs,
):
    l, r, c = (lax.axis_index(a) for a in ("layer", "row", "col"))
    slots, edge, _ = values.shape
    blocks = x_ref.shape[0]
    halves = edge // 128
    nchunk = slots // PIECE
    early = nchunk // 2
    cuts = [(sum(CUTS[:i]), n) for i, n in enumerate(CUTS)]
    f32, bf16 = jnp.float32, jnp.bfloat16

    def remote(src, dst, ss, rs, ll, rr, cc):
        return pltpu.make_async_remote_copy(
            src_ref=src, dst_ref=dst, send_sem=ss, recv_sem=rs,
            device_id=(ll, rr, cc), device_id_type=pl.DeviceIdType.MESH,
        )

    in_d = pltpu.make_async_copy(dang_hbm, dang_in, sem_in.at[0])
    in_x = pltpu.make_async_copy(start_hbm, start_in, sem_in.at[1])
    vcopies = [
        pltpu.make_async_copy(
            values_hbm.at[pl.ds(k * PIECE, PIECE)], values.at[pl.ds(k * PIECE, PIECE)], sem_v.at[k]
        )
        for k in range(nchunk)
    ]
    small = [
        pltpu.make_async_copy(src, dst, sem_in.at[2 + i])
        for i, (src, dst) in enumerate(
            [(rows_hbm, rows_ref), (cols_hbm, cols_ref), (count_hbm, count_ref)])
    ]
    in_x.start()
    in_d.start()
    for cp in small:
        cp.start()
    for cp in vcopies:
        cp.start(priority=1)

    peers = [(dr, dc) for dr in range(nr) for dc in range(nc) if (dr, dc) != (0, 0)]
    barrier = pltpu.get_barrier_semaphore()
    def tell(sem, *to):
        pl.semaphore_signal(sem, inc=1, device_id=to, device_id_type=pl.DeviceIdType.MESH)

    for d in range(1, nr):
        tell(barrier, l, lax.rem(r + d, nr), c)
    for d in range(1, nc):
        @pl.when(c + d < nc)
        def _():
            for rr in range(nr):
                tell(barrier, l, rr, c + d)

    @pl.when(l < nl - 1)
    def _():
        tell(barrier, l + 1, r, c)

    for cp in small:
        cp.wait()
    live = lax.broadcasted_iota(jnp.int32, (1, slots), 1) < count_ref[...]
    rows = jnp.where(live, rows_ref[...], -1)
    cols = jnp.where(live, cols_ref[...], -1)
    pad = jnp.full((1, 128 - slots), -1, jnp.int32)
    row_send[...] = jnp.concatenate([rows, pad], axis=1).astype(f32)
    col_send[...] = jnp.concatenate([cols, pad], axis=1).astype(f32)

    eye = lax.broadcasted_iota(jnp.int32, (slots, slots), 0) == lax.broadcasted_iota(
        jnp.int32, (slots, slots), 1)

    def upright(tab):
        return jnp.sum(
            jnp.where(eye, jnp.broadcast_to(tab, (slots, slots)), 0.0), axis=1, keepdims=True)

    colv = upright(cols_ref[...].astype(f32))
    for d in range(nr):
        base = lax.rem(r - d + nr, nr) * blocks
        at = (lax.broadcasted_iota(jnp.int32, (slots, blocks), 1) + base).astype(f32)
        ohcol[d] = jnp.where(colv == at, 1.0, 0.0).astype(bf16)

    ones = jnp.ones((CHUNK, edge), bf16)
    rid = lax.broadcasted_iota(jnp.int32, (PIECE, edge), 0)

    def column_sum(k):
        vcopies[k].wait()
        acc = jnp.zeros((PIECE, edge), f32)
        for s in range(PIECE):
            acc = jnp.where(rid == s, dot(ones, values[k * PIECE + s])[0:PIECE], acc)
        colsum[k] = acc

    def transpose(k):
        for s in range(k * PIECE, (k + 1) * PIECE):
            vt[s] = values[s].T

    pl.semaphore_wait(barrier, nr - 1 + nr * c + (l > 0).astype(jnp.int32))
    for d in range(1, nc):
        @pl.when(c >= d)
        def _():
            for rr in range(nr):
                tell(ready.at[0], l, rr, c - d)

    @pl.when(l > 0)
    def _():
        tell(ready.at[1], l - 1, r, c)

    in_x.wait()
    in_d.wait()
    for h in range(halves):
        x_ref[:, h * 128 : (h + 1) * 128] = start_in[pl.ds(h, blocks, stride=halves), :]
    column_sum(0)

    order = []
    first, last = jnp.int32(0), jnp.int32(nc - 1)
    for _ in range(nc - 1):
        left = (c - first >= last - c).astype(jnp.int32)
        order.append(left * first + (1 - left) * last)
        first, last = first + left, last - (1 - left)
    far = [(cc, lax.rem(cc - c + nc, nc)) for cc in order]
    far_peers = [(dr, cc, d) for cc, d in far for dr in range(nr)]
    far_peers += [(dr, c, 0) for dr in range(1, nr)]
    sent = []

    px, pd, pc, pcs, prow = [], [], [], [], []
    for d in range(1, nr):
        rr = lax.rem(r + d, nr)
        px.append(remote(start_in, px_recv.at[d], px_ss.at[d], px_rs.at[d], l, rr, c))
        pd.append(remote(dang_in, pd_recv.at[d], pd_ss.at[d], pd_rs.at[d], l, rr, c))
        pc.append(remote(col_send, col_recv.at[d], col_ss.at[d], col_rs.at[d], l, rr, c))
        pcs.append([
            remote(colsum.at[k], cs_recv.at[d, k], cs_ss.at[d, k], cs_rs.at[d, k], l, rr, c)
            for k in range(nchunk)
        ])
    for cc, d in far:
        prow.append(remote(row_send, row_recv.at[d], row_ss.at[d], row_rs.at[d], l, r, cc))
    for cp in px + pd + pc + [q[0] for q in pcs]:
        cp.start()

    def start_where(pairs):
        for cp, cond in pairs:
            @pl.when(cond)
            def _():
                cp.start()

    start_where([(cp, cc < c) for cp, (cc, _) in zip(prow, far)])

    def spill_copies(t):
        return (
            remote(sp_send.at[t], sp_recv.at[t, 0], sp_ss.at[t, 0], sp_rs.at[t, 0], l + 1, r, c),
            remote(sp_send.at[t], sp_recv.at[t, 1], sp_ss.at[t, 1], sp_rs.at[t, 1], l - 1, r, c),
        )

    spread = jnp.where((l == 0) | (l == nl - 1), 1.0, 0.5).astype(f32) * coupling

    def send_spill(t, x, when):
        if x is not None:
            sp_send[t] = (x * spread).astype(sp_send.dtype)
        up, down = spill_copies(t)

        @pl.when((l < nl - 1) & when)
        def _():
            up.start()

        @pl.when((l > 0) & when)
        def _():
            down.start()

    @pl.when(l == 0)
    def _():
        for t in range(ITERS):
            sp_recv[t, 0] = jnp.zeros((blocks, edge), sp_recv.dtype)

    @pl.when(l == nl - 1)
    def _():
        for t in range(ITERS):
            sp_recv[t, 1] = jnp.zeros((blocks, edge), sp_recv.dtype)

    for k in range(1, nchunk):
        column_sum(k)
        for q in pcs:
            q[k].start()
    for k in range(early):
        transpose(k)

    def hot(tab, rr):
        at = (lax.broadcasted_iota(jnp.int32, (blocks, slots), 0) + rr * blocks).astype(f32)
        return jnp.where(
            jnp.broadcast_to(tab[0:1, 0:slots], (blocks, slots)) == at, 1.0, 0.0).astype(bf16)

    def spread_sums(oh, sums):
        hi, lo = split(sums.reshape(slots, edge))
        return dot(oh, hi) + dot(oh, lo)

    def piece(buf, h):
        return buf[pl.ds(h, blocks, stride=halves), :]

    whose = [lax.rem(r - d + nr, nr) for d in range(nr)]
    near = [spread_sums(hot(col_send, rr), colsum[...]) for rr in whose]
    for cp in px + pd + pc:
        cp.wait_recv()
    peer_x = {d: jnp.concatenate([piece(px_recv.at[d], h) for h in range(halves)], axis=1)
              for d in range(1, nr)}
    keeps = {d: 1.0 - jnp.concatenate(
        [piece(pd_recv.at[d] if d else dang_in, h) for h in range(halves)], axis=1).astype(f32)
        for d in range(nr)}
    hots = [[hot(col_recv[e], rr) for e in range(1, nr)] for rr in whose]
    for e in range(nr):
        tab = colv if e == 0 else upright(col_recv[e][0:1, 0:slots])
        at = (lax.broadcasted_iota(jnp.int32, (slots, blocks), 1) + r * blocks).astype(f32)
        ohq[e * slots : (e + 1) * slots] = jnp.where(tab == at, 1.0, 0.0).astype(bf16)
    for q in pcs:
        for cp in q:
            cp.wait_recv()
    @pl.when(l < nl - 1)
    def _():
        pl.semaphore_wait(ready.at[1], 1)

    send_spill(0, x_ref[...], r >= 0)
    for d in range(nr):
        deg = near[d]
        for e in range(1, nr):
            deg = deg + spread_sums(hots[d][e - 1], cs_recv[e])
        inv = 1.0 / (keeps[d] * deg + 1.0)
        kinv = keeps[d] * inv
        if d == 0:
            inv_ref[...] = inv
            kinv_ref[...] = kinv
        else:
            sc_recv[d] = (peer_x[d] * kinv).astype(bf16)

    def row_onehot(tabs):
        tab = jnp.concatenate([tab[0:1, 0:slots] for tab in tabs], axis=1)
        shape = (blocks, tab.shape[1])
        at = (lax.broadcasted_iota(jnp.int32, shape, 0) + c * blocks).astype(f32)
        return jnp.where(jnp.broadcast_to(tab, shape) == at, 1.0, 0.0).astype(bf16)

    def pick_copies(t):
        return [
            remote(pk_send.at[t, d], pk_recv.at[t, d], sc_ss.at[t, d], sc_rs.at[t, d],
                   l, lax.rem(r + d, nr), c)
            for d in range(1, nr)
        ]

    def picks(t):
        if t == 0:
            acc = dot(ohcol[0], (x_ref[...] * kinv_ref[...]).astype(bf16))
            for d in range(1, nr):
                acc = acc + dot(ohcol[d], sc_recv[d])
            return acc.astype(bf16)
        acc = pk_own[...]
        for d, cp in enumerate(pick_copies(t), 1):
            cp.wait_recv()
            acc = acc + pk_recv[t, d].astype(f32)
        return acc.astype(bf16)

    def products(t, ma):
        picked = picks(t)
        if t > 0:
            send_spill(t, None, lax.rem(r, 2) == 0)
        def piece_copy(k, cc, d):
            at, n = cuts[k]
            return remote(
                pr_send.at[t, pl.ds(at, n)], pr_recv.at[t, d, pl.ds(at, n)], pr_ss.at[t, d, k],
                pr_rs.at[t, d, k], l, r, cc)

        pr = []
        for k, (at, n) in enumerate(cuts):
            for at in range(at, at + n, PIECE):
                base = at // CHUNK * CHUNK
                lhs = picked[base : base + CHUNK]
                acc = jnp.zeros((PIECE, edge), f32)
                for s in range(PIECE):
                    if t == 0 and at >= early * PIECE:
                        res = lax.dot_general(
                            lhs, values[at + s], (((1,), (1,)), ((), ())),
                            preferred_element_type=f32)
                    else:
                        res = dot(lhs, vt[at + s])
                    acc = jnp.where(rid == s, res[at - base : at - base + PIECE], acc)
                own_prod[at : at + PIECE] = acc
                pr_send[t, at : at + PIECE] = acc.astype(pr_send.dtype)
            if t == 0 and k == 0:
                @pl.when(c < nc - 1)
                def _():
                    pl.semaphore_wait(ready.at[0], nr * (nc - 1 - c))

                start_where([(cp, cc > c) for cp, (cc, _) in zip(prow, far)])
                start_where([(cp, cc > c) for cp, (_, cc, _) in zip(ma, far_peers)])
            pr += [piece_copy(k, *to) for to in (far[:-1] if k < len(cuts) - 1 else far)]
            for cp in pr[-len(far) + (k < len(cuts) - 1) :]:
                cp.start()
            if t > 0 and k == 0:
                @pl.when(lax.rem(r, 2) == 0)
                def _():
                    for cp in ma:
                        cp.start()

        for k in range(len(cuts) - 1):
            pr.append(piece_copy(k, *far[-1]))
            pr[-1].start()
        sent.extend(pr)

    def masses(t):
        mass_own = jnp.sum(fold(x_ref[...] * inv_ref[...]), axis=0, keepdims=True)
        ma_send[t] = mass_own
        ma = []
        for i, (dr, cc, dc) in enumerate(far_peers):
            slot = dr * nc + dc - 1
            ma.append(remote(ma_send.at[t], ma_recv.at[t, slot], ma_ss.at[t, slot],
                             ma_rs.at[t, slot], l, lax.rem(r + dr, nr), cc))
        if t == 0:
            start_where([(cp, cc <= c) for cp, (_, cc, _) in zip(ma, far_peers)])
        else:
            @pl.when(lax.rem(r, 2) == 1)
            def _():
                for cp in ma:
                    cp.start()

        sent.extend(ma)
        return mass_own, ma

    def note_change(t):
        part = jnp.sum(diff[t], axis=0, keepdims=True)
        lane = lax.broadcasted_iota(jnp.int32, (1, 128), 1)
        old = chg[...] if t else jnp.zeros((1, 128), f32)
        chg[...] = jnp.where(lane == t, jnp.sum(part, axis=1, keepdims=True), old)

    def step(t, mass_own, ma):
        products(t, ma)
        if t > 0:
            note_change(t - 1)
        if t == 0:
            for k in range(early, nchunk):
                transpose(k)
            for cp in prow:
                cp.wait_recv()
            for part, tabs in enumerate([[row_send], [row_recv.at[d] for d in range(1, nc)]]):
                oh = row_onehot(tabs)
                ref = hot_far if part else hot_own
                ref[nr * slots :] = oh
                ref[0 : nr * slots] = dot(ohq[...], oh).astype(bf16)
            khi, klo = split(kinv_ref[...])
            kg_ref[...] = dot(ohq[...], khi) + dot(ohq[...], klo)

        phi, plo = split(own_prod[...])
        last = t == ITERS - 1
        npick = 0 if last else nr * slots
        skip = nr * slots - npick
        near_sum = dot(hot_own[skip:], phi) + dot(hot_own[skip:], plo)

        up, down = spill_copies(t)

        @pl.when(l > 0)
        def _():
            up.wait_recv()

        @pl.when(l < nl - 1)
        def _():
            down.wait_recv()

        arrive = sp_recv[t, 0].astype(f32) + sp_recv[t, 1].astype(f32)
        mass = mass_own
        for cp in ma:
            cp.wait_recv()
        for i in range(len(peers)):
            mass = mass + ma_recv[t, i]
        flat = damping * (1.0 - coupling) * (jnp.sum(mass) / nodes) + (1.0 - damping)
        rest = damping * arrive + flat
        if not last:
            restg = damping * (dot(ohq[...], sp_recv[t, 0]) + dot(ohq[...], sp_recv[t, 1])) + flat

        gain = damping * (1.0 - coupling)
        if not last:
            near_pick = gain * near_sum[0:npick] + restg
        near_walk = gain * near_sum[npick:] + rest
        for d in range(1, nc):
            for k, (at, n) in enumerate(cuts):
                remote(pr_send.at[t, pl.ds(at, n)], pr_recv.at[t, d, pl.ds(at, n)],
                       pr_ss.at[t, d, k], pr_rs.at[t, d, k],
                       l, r, lax.rem(c + d, nc)).wait_recv()
        far_sum = dot(hot_far[skip:], pr_recv[t, 1:nc].reshape((nc - 1) * slots, edge))
        if not last:
            pk = kg_ref[...] * (gain * far_sum[0:npick] + near_pick)
            for d in range(1, nr):
                pk_send[t + 1, d] = pk[d * slots : (d + 1) * slots].astype(bf16)
            pk_own[...] = pk[0:slots].astype(bf16).astype(f32)
            cps = pick_copies(t + 1)
            for cp in cps:
                cp.start()
            sent.extend(cps)
        x = x_ref[...]
        updated = gain * far_sum[npick:] + near_walk
        x_ref[...] = updated
        diff[t] = fold(jnp.abs(updated - x))
        if last:
            note_change(t)
            return None
        send_spill(t + 1, updated, lax.rem(r, 2) == 1)
        return masses(t + 1)

    carry = masses(0)
    for t in range(ITERS):
        carry = step(t, *carry)

    rs_send[...] = chg[...]
    rs = []
    for dr, cc, dc in far_peers:
        i = dr * nc + dc - 1
        cp = remote(rs_send, rs_recv.at[i], rs_ss.at[i], rs_rs.at[i],
                    l, lax.rem(r + dr, nr), cc)
        cp.start()
        rs.append(cp)
    for h in range(halves):
        ranks_ref[pl.ds(h, blocks, stride=halves), :] = x_ref[:, h * 128 : (h + 1) * 128]
    for cp in px + pd + pc + prow + [e for q in pcs for e in q] + sent:
        cp.wait_send()
    ups = [spill_copies(t) for t in range(ITERS)]

    @pl.when(l < nl - 1)
    def _():
        for up, _ in ups:
            up.wait_send()

    @pl.when(l > 0)
    def _():
        for _, down in ups:
            down.wait_send()

    total = rs_send[...]
    for cp in rs:
        cp.wait_recv()
    for i in range(len(peers)):
        total = total + rs_recv[i]
    resid_ref[...] = total
    for cp in rs:
        cp.wait_send()


def scoped(sems, *args):
    pl.run_scoped(lambda *refs: kernel(*args, *refs), *sems)


def finish(ranks_in, resid_in, ranks_ref, resid_ref):
    ranks_ref[...] = ranks_in[...]
    resid_ref[...] = resid_in[:, 0:ITERS]


def local(block_values, block_rows, block_cols, block_count, dangling, start_ranks):
    span = start_ranks.shape[-1]
    nl, nr, nc = (lax.axis_size(a) for a in ("layer", "row", "col"))
    slots, edge = block_values.shape[3], block_values.shape[-1]
    blocks = span // edge
    nchunk = slots // PIECE
    nodes = nr * nc * span
    npeer = nr * nc - 1
    f32, bf16 = jnp.float32, jnp.bfloat16
    vm, dma = pltpu.VMEM, pltpu.SemaphoreType.DMA
    big = (blocks, edge)
    PT, ST = bf16, bf16
    scratch = [
        vm((slots, edge, edge), bf16), vm((slots, edge, edge), bf16), vm((span // 128, 128), jnp.int32), vm((span // 128, 128), f32),
        vm(big, f32), vm(big, f32), vm(big, f32),
        vm((nchunk, PIECE, edge), f32), vm((nr, slots, blocks), bf16),
        vm((slots, edge), f32), vm((ITERS, 8, 128), f32), vm((1, 128), f32),
        vm((slots, edge), f32), vm((ITERS, nr, slots, edge), bf16), vm((ITERS, nr, slots, edge), bf16),
        vm((nr * slots, edge), f32), vm((nr * slots + blocks, slots), bf16),
        vm((nr * slots + blocks, (nc - 1) * slots), bf16), vm((nr * slots, blocks), bf16),
        vm((nr, span // 128, 128), f32), vm((nr, span // 128, 128), jnp.int32),
        vm((1, 128), f32), vm((nr, 1, 128), f32), vm((nr, nchunk, PIECE, edge), f32),
        vm((1, 128), f32), vm((nc, 1, 128), f32),
        vm((nr,) + big, bf16),
        vm((ITERS, 1, 128), f32), vm((ITERS, npeer, 1, 128), f32),
        vm((ITERS, slots, edge), PT), vm((ITERS, nc, slots, edge), PT),
        vm((ITERS,) + big, ST), vm((ITERS, 2) + big, ST),
        vm((1, 128), f32), vm((npeer, 1, 128), f32),
        vm((1, slots), jnp.int32), vm((1, slots), jnp.int32), vm((1, 1), jnp.int32),
    ]
    sems = [
        dma((5,)), dma((nchunk,)),
        dma((nr,)), dma((nr,)), dma((nr,)), dma((nr,)), dma((nr,)), dma((nr,)),
        dma((nr, nchunk)), dma((nr, nchunk)), dma((nc,)), dma((nc,)),
        dma((ITERS, nr)), dma((ITERS, nr)), dma((ITERS, npeer)), dma((ITERS, npeer)),
        pltpu.SemaphoreType.REGULAR((2,)),
        dma((ITERS, nc, len(CUTS))), dma((ITERS, nc, len(CUTS))),
        dma((ITERS, 2)), dma((ITERS, 2)), dma((npeer,)), dma((npeer,)),
    ]
    hbm = pl.BlockSpec(memory_space=pltpu.HBM)
    vmem = pl.BlockSpec(memory_space=pltpu.VMEM)
    ranks, resid = pl.pallas_call(
        functools.partial(scoped, sems, nl, nr, nc, nodes),
        out_shape=(
            pltpu.VMEM((span // 128, 128), f32),
            pltpu.VMEM((1, 128), f32),
        ),
        in_specs=[hbm] * 6,
        out_specs=(vmem, vmem),
        scratch_shapes=scratch,
        compiler_params=pltpu.CompilerParams(collective_id=0, has_side_effects=True),
    )(
        block_values.reshape(slots, edge, edge),
        block_rows.reshape(1, slots),
        block_cols.reshape(1, slots),
        block_count.reshape(1, 1),
        dangling.reshape(span // 128, 128),
        start_ranks.reshape(span // 128, 128),
    )
    ranks, resid = pl.pallas_call(
        finish,
        out_shape=(
            jax.ShapeDtypeStruct((span // 128, 128), f32),
            jax.ShapeDtypeStruct((1, ITERS), f32),
        ),
        in_specs=[vmem, vmem],
        out_specs=(vmem, vmem),
        compiler_params=pltpu.CompilerParams(vmem_limit_bytes=4 * 1024 * 1024),
    )(ranks, resid)
    return ranks.reshape(1, 1, 1, span), resid.T


def solution(mesh):
    placed = (
        P("layer", "row", "col", None, None, None),
        P("layer", "row", "col", None),
        P("layer", "row", "col", None),
        P("layer", "row", "col"),
        P("layer", "row", "col", None),
        P("layer", "row", "col", None),
    )
    return jax.shard_map(
        local,
        mesh=mesh,
        in_specs=placed,
        out_specs=(P("layer", "row", "col", None), P(None, "layer")),
        check_vma=False,
    )
```

```python
import functools

import jax
import jax.numpy as jnp
from jax import lax
from jax.experimental import pallas as pl
from jax.experimental.pallas import tpu as pltpu
from jax.sharding import PartitionSpec as P

ITERS = 3
CHUNK = 16
PIECE = 8
CUTS = (16, 16)

damping = 0.85
coupling = 0.3


def fold(v):
    rows, lanes = v.shape
    acc = v[:, 0:128]
    for h in range(1, lanes // 128):
        acc = acc + v[:, h * 128 : (h + 1) * 128]
    return jnp.sum(acc.reshape(rows // 8, 8, 128), axis=0)


def split(v):
    hi = v.astype(jnp.bfloat16)
    lo = (v - hi.astype(jnp.float32)).astype(jnp.bfloat16)
    return hi, lo


def dot(a, b):
    return jnp.dot(a, b, preferred_element_type=jnp.float32)


def kernel(
    nl, nr, nc, nodes,
    values_hbm, rows_hbm, cols_hbm, count_hbm, dang_hbm, start_hbm,
    ranks_ref, resid_ref,
    values, vt, dang_in, start_in, x_ref, inv_ref, kinv_ref,
    kg_pair, kinv_pair, hot_pair, rowp_recv, pp_recv, rg_send, rg_recv,
    colsum, ohcol, own_prod, diff, chg,
    pk_own, pk_send, pk_recv, kg_ref, hot_own, hot_far, ohq,
    px_recv, pd_recv, col_send, col_recv, cs_recv, row_send, row_recv,
    sc_recv, ma_send, ma_recv,
    pr_send, pr_recv, sp_send, sp_recv, rs_send, rs_recv,
    rows_ref, cols_ref, count_ref,
    sem_in, sem_v,
    px_ss, px_rs, pd_ss, pd_rs, col_ss, col_rs, cs_ss, cs_rs, row_ss, row_rs, sc_ss, sc_rs, ma_ss, ma_rs,
    ready, rowp_ss, rowp_rs, pp_ss, pp_rs, rg_ss, rg_rs,
    pr_ss, pr_rs, sp_ss, sp_rs, rs_ss, rs_rs,
):
    l, r, c = (lax.axis_index(a) for a in ("layer", "row", "col"))
    slots, edge, _ = values.shape
    blocks = x_ref.shape[0]
    halves = edge // 128
    nchunk = slots // PIECE
    early = nchunk * 3 // 4
    gives = lax.rem(r, 2) == 0
    takes = lax.rem(r, 2) == 1
    mate = lax.rem(r + 1, nr)
    gain = damping * (1.0 - coupling)
    cuts = [(sum(CUTS[:i]), n) for i, n in enumerate(CUTS)]
    f32, bf16 = jnp.float32, jnp.bfloat16

    def remote(src, dst, ss, rs, ll, rr, cc):
        return pltpu.make_async_remote_copy(
            src_ref=src, dst_ref=dst, send_sem=ss, recv_sem=rs,
            device_id=(ll, rr, cc), device_id_type=pl.DeviceIdType.MESH,
        )

    in_d = pltpu.make_async_copy(dang_hbm, dang_in, sem_in.at[0])
    in_x = pltpu.make_async_copy(start_hbm, start_in, sem_in.at[1])
    vcopies = [
        pltpu.make_async_copy(
            values_hbm.at[pl.ds(k * PIECE, PIECE)], values.at[pl.ds(k * PIECE, PIECE)], sem_v.at[k]
        )
        for k in range(nchunk)
    ]
    small = [
        pltpu.make_async_copy(src, dst, sem_in.at[2 + i])
        for i, (src, dst) in enumerate(
            [(rows_hbm, rows_ref), (cols_hbm, cols_ref), (count_hbm, count_ref)])
    ]
    in_x.start()
    in_d.start()
    for cp in small:
        cp.start()
    for cp in vcopies:
        cp.start(priority=1)

    peers = [(dr, dc) for dr in range(nr) for dc in range(nc) if (dr, dc) != (0, 0)]
    barrier = pltpu.get_barrier_semaphore()
    def tell(sem, *to):
        pl.semaphore_signal(sem, inc=1, device_id=to, device_id_type=pl.DeviceIdType.MESH)

    for d in range(1, nr):
        tell(barrier, l, lax.rem(r + d, nr), c)
    for d in range(1, nc):
        @pl.when(c + d < nc)
        def _():
            for rr in range(nr):
                tell(barrier, l, rr, c + d)

    @pl.when(l < nl - 1)
    def _():
        tell(barrier, l + 1, r, c)

    for cp in small:
        cp.wait()
    live = lax.broadcasted_iota(jnp.int32, (1, slots), 1) < count_ref[...]
    rows = jnp.where(live, rows_ref[...], -1)
    cols = jnp.where(live, cols_ref[...], -1)
    pad = jnp.full((1, 128 - slots), -1, jnp.int32)
    row_send[...] = jnp.concatenate([rows, pad], axis=1).astype(f32)
    col_send[...] = jnp.concatenate([cols, pad], axis=1).astype(f32)

    eye = lax.broadcasted_iota(jnp.int32, (slots, slots), 0) == lax.broadcasted_iota(
        jnp.int32, (slots, slots), 1)

    def upright(tab):
        return jnp.sum(
            jnp.where(eye, jnp.broadcast_to(tab, (slots, slots)), 0.0), axis=1, keepdims=True)

    colv = upright(cols_ref[...].astype(f32))
    for d in range(nr):
        base = lax.rem(r - d + nr, nr) * blocks
        at = (lax.broadcasted_iota(jnp.int32, (slots, blocks), 1) + base).astype(f32)
        ohcol[d] = jnp.where(colv == at, 1.0, 0.0).astype(bf16)

    ones = jnp.ones((CHUNK, edge), bf16)
    rid = lax.broadcasted_iota(jnp.int32, (PIECE, edge), 0)

    def column_sum(k):
        vcopies[k].wait()
        acc = jnp.zeros((PIECE, edge), f32)
        for s in range(PIECE):
            acc = jnp.where(rid == s, dot(ones, values[k * PIECE + s])[0:PIECE], acc)
        colsum[k] = acc

    def transpose(k):
        for s in range(k * PIECE, (k + 1) * PIECE):
            vt[s] = values[s].T

    pl.semaphore_wait(barrier, nr - 1 + nr * c + (l > 0).astype(jnp.int32))
    for d in range(1, nc):
        @pl.when(c >= d)
        def _():
            for rr in range(nr):
                tell(ready.at[0], l, rr, c - d)

    @pl.when(l > 0)
    def _():
        tell(ready.at[1], l - 1, r, c)

    in_x.wait()
    in_d.wait()
    for h in range(halves):
        x_ref[:, h * 128 : (h + 1) * 128] = start_in[pl.ds(h, blocks, stride=halves), :]
    column_sum(0)

    order = []
    first, last = jnp.int32(0), jnp.int32(nc - 1)
    for _ in range(nc - 1):
        left = (c - first >= last - c).astype(jnp.int32)
        order.append(left * first + (1 - left) * last)
        first, last = first + left, last - (1 - left)
    far = [(cc, lax.rem(cc - c + nc, nc)) for cc in order]
    far_peers = [(dr, cc, d) for cc, d in far for dr in range(nr)]
    far_peers += [(dr, c, 0) for dr in range(1, nr)]
    sent = []

    px, pd, pc, pcs, prow = [], [], [], [], []
    for d in range(1, nr):
        rr = lax.rem(r + d, nr)
        px.append(remote(start_in, px_recv.at[d], px_ss.at[d], px_rs.at[d], l, rr, c))
        pd.append(remote(dang_in, pd_recv.at[d], pd_ss.at[d], pd_rs.at[d], l, rr, c))
        pc.append(remote(col_send, col_recv.at[d], col_ss.at[d], col_rs.at[d], l, rr, c))
        pcs.append([
            remote(colsum.at[k], cs_recv.at[d, k], cs_ss.at[d, k], cs_rs.at[d, k], l, rr, c)
            for k in range(nchunk)
        ])
    for cc, d in far:
        prow.append(remote(row_send, row_recv.at[d], row_ss.at[d], row_rs.at[d], l, r, cc))
    for cp in px + pd + pc + [q[0] for q in pcs]:
        cp.start()

    def start_where(pairs):
        for cp, cond in pairs:
            @pl.when(cond)
            def _():
                cp.start()

    start_where([(cp, cc < c) for cp, (cc, _) in zip(prow, far)])
    everyone = far + [(c, 0)]
    mate_rows = [
        remote(row_send, rowp_recv.at[d], rowp_ss.at[d], rowp_rs.at[d], l, mate, cc)
        for cc, d in everyone
    ]
    mate_prods = [
        remote(pr_send.at[0], pp_recv.at[d], pp_ss.at[d], pp_rs.at[d], l, mate, cc)
        for cc, d in everyone
    ]
    mate_rest = remote(rg_send, rg_recv, rg_ss.at[0], rg_rs.at[0], l, mate, c)
    start_where([(cp, gives & (cc <= c)) for cp, (cc, _) in zip(mate_rows, everyone)])

    def spill_copies(t):
        return (
            remote(sp_send.at[t], sp_recv.at[t, 0], sp_ss.at[t, 0], sp_rs.at[t, 0], l + 1, r, c),
            remote(sp_send.at[t], sp_recv.at[t, 1], sp_ss.at[t, 1], sp_rs.at[t, 1], l - 1, r, c),
        )

    spread = jnp.where((l == 0) | (l == nl - 1), 1.0, 0.5).astype(f32) * coupling

    def send_spill(t, x, when):
        if x is not None:
            sp_send[t] = (x * spread).astype(sp_send.dtype)
        up, down = spill_copies(t)

        @pl.when((l < nl - 1) & when)
        def _():
            up.start()

        @pl.when((l > 0) & when)
        def _():
            down.start()

    @pl.when(l == 0)
    def _():
        for t in range(ITERS):
            sp_recv[t, 0] = jnp.zeros((blocks, edge), sp_recv.dtype)

    @pl.when(l == nl - 1)
    def _():
        for t in range(ITERS):
            sp_recv[t, 1] = jnp.zeros((blocks, edge), sp_recv.dtype)

    for k in range(1, nchunk):
        column_sum(k)
        for q in pcs:
            q[k].start()
    for k in range(early):
        transpose(k)

    def hot(tab, rr):
        at = (lax.broadcasted_iota(jnp.int32, (blocks, slots), 0) + rr * blocks).astype(f32)
        return jnp.where(
            jnp.broadcast_to(tab[0:1, 0:slots], (blocks, slots)) == at, 1.0, 0.0).astype(bf16)

    def spread_sums(oh, sums):
        hi, lo = split(sums.reshape(slots, edge))
        return dot(oh, hi) + dot(oh, lo)

    def piece(buf, h):
        return buf[pl.ds(h, blocks, stride=halves), :]

    whose = [lax.rem(r - d + nr, nr) for d in range(nr)]
    near = [spread_sums(hot(col_send, rr), colsum[...]) for rr in whose]
    for cp in px + pd + pc:
        cp.wait_recv()
    peer_x = {d: jnp.concatenate([piece(px_recv.at[d], h) for h in range(halves)], axis=1)
              for d in range(1, nr)}
    keeps = {d: 1.0 - jnp.concatenate(
        [piece(pd_recv.at[d] if d else dang_in, h) for h in range(halves)], axis=1).astype(f32)
        for d in range(nr)}
    hots = [[hot(col_recv[e], rr) for e in range(1, nr)] for rr in whose]
    for e in range(nr):
        tab = colv if e == 0 else upright(col_recv[e][0:1, 0:slots])
        at = (lax.broadcasted_iota(jnp.int32, (slots, blocks), 1) + r * blocks).astype(f32)
        ohq[e * slots : (e + 1) * slots] = jnp.where(tab == at, 1.0, 0.0).astype(bf16)
    for q in pcs:
        for cp in q:
            cp.wait_recv()
    @pl.when(l < nl - 1)
    def _():
        pl.semaphore_wait(ready.at[1], 1)

    send_spill(0, x_ref[...], r >= 0)
    for d in range(nr):
        deg = near[d]
        for e in range(1, nr):
            deg = deg + spread_sums(hots[d][e - 1], cs_recv[e])
        inv = 1.0 / (keeps[d] * deg + 1.0)
        kinv = keeps[d] * inv
        if d == 0:
            inv_ref[...] = inv
            kinv_ref[...] = kinv
        else:
            sc_recv[d] = (peer_x[d] * kinv).astype(bf16)
            if d == 1:
                kinv_pair[...] = kinv

    def row_onehot(tabs):
        tab = jnp.concatenate([tab[0:1, 0:slots] for tab in tabs], axis=1)
        shape = (blocks, tab.shape[1])
        at = (lax.broadcasted_iota(jnp.int32, shape, 0) + c * blocks).astype(f32)
        return jnp.where(jnp.broadcast_to(tab, shape) == at, 1.0, 0.0).astype(bf16)

    def pick_copies(t):
        return [
            remote(pk_send.at[t, d], pk_recv.at[t, d], sc_ss.at[t, d], sc_rs.at[t, d],
                   l, lax.rem(r + d, nr), c)
            for d in range(1, nr)
        ]

    def picks(t):
        if t == 0:
            acc = dot(ohcol[0], (x_ref[...] * kinv_ref[...]).astype(bf16))
            for d in range(1, nr):
                acc = acc + dot(ohcol[d], sc_recv[d])
            return acc.astype(bf16)
        acc = pk_own[...]
        if t == 1:
            @pl.when(takes)
            def _():
                for cp in mate_prods + [mate_rest]:
                    cp.wait_recv()
                pw = dot(hot_pair[...], pp_recv[...].reshape(nc * slots, edge))
                pk_recv[1, 1] = (kg_pair[...] * (gain * pw + rg_recv[...])).astype(bf16)

        for d, cp in enumerate(pick_copies(t), 1):
            if t == 1 and d == 1:
                @pl.when(gives)
                def _():
                    cp.wait_recv()
            else:
                cp.wait_recv()
            acc = acc + pk_recv[t, d].astype(f32)
        return acc.astype(bf16)

    def products(t, ma):
        picked = picks(t)
        if t > 0:
            send_spill(t, None, lax.rem(r, 2) == 0)
        def piece_copy(k, cc, d):
            at, n = cuts[k]
            return remote(
                pr_send.at[t, pl.ds(at, n)], pr_recv.at[t, d, pl.ds(at, n)], pr_ss.at[t, d, k],
                pr_rs.at[t, d, k], l, r, cc)

        pr = []
        for k, (at, n) in enumerate(cuts):
            for at in range(at, at + n, PIECE):
                base = at // CHUNK * CHUNK
                lhs = picked[base : base + CHUNK]
                acc = jnp.zeros((PIECE, edge), f32)
                for s in range(PIECE):
                    if t == 0 and at >= early * PIECE:
                        res = lax.dot_general(
                            lhs, values[at + s], (((1,), (1,)), ((), ())),
                            preferred_element_type=f32)
                    else:
                        res = dot(lhs, vt[at + s])
                    acc = jnp.where(rid == s, res[at - base : at - base + PIECE], acc)
                own_prod[at : at + PIECE] = acc
                pr_send[t, at : at + PIECE] = acc.astype(pr_send.dtype)
            if t == 0 and k == 0:
                @pl.when(c < nc - 1)
                def _():
                    pl.semaphore_wait(ready.at[0], nr * (nc - 1 - c))

                start_where([(cp, cc > c) for cp, (cc, _) in zip(prow, far)])
                start_where([(cp, gives & (cc > c)) for cp, (cc, _) in zip(mate_rows, everyone)])
                start_where([(cp, cc > c) for cp, (_, cc, _) in zip(ma, far_peers)])
            pr += [piece_copy(k, *to) for to in (far[:-1] if k < len(cuts) - 1 else far)]
            for cp in pr[-len(far) + (k < len(cuts) - 1) :]:
                cp.start()
        for k in range(len(cuts) - 1):
            pr.append(piece_copy(k, *far[-1]))
            pr[-1].start()
        sent.extend(pr)
        if t == 0:
            @pl.when(gives)
            def _():
                for cp in mate_prods:
                    cp.start()


    def masses(t):
        mass_own = jnp.sum(fold(x_ref[...] * inv_ref[...]), axis=0, keepdims=True)
        ma_send[t] = mass_own
        ma = []
        for i, (dr, cc, dc) in enumerate(far_peers):
            slot = dr * nc + dc - 1
            ma.append(remote(ma_send.at[t], ma_recv.at[t, slot], ma_ss.at[t, slot],
                             ma_rs.at[t, slot], l, lax.rem(r + dr, nr), cc))
        if t == 0:
            start_where([(cp, cc <= c) for cp, (_, cc, _) in zip(ma, far_peers)])
        else:
            for cp in ma:
                cp.start()
        sent.extend(ma)
        return mass_own, ma

    def note_change(t):
        part = jnp.sum(diff[t], axis=0, keepdims=True)
        lane = lax.broadcasted_iota(jnp.int32, (1, 128), 1)
        old = chg[...] if t else jnp.zeros((1, 128), f32)
        chg[...] = jnp.where(lane == t, jnp.sum(part, axis=1, keepdims=True), old)

    def step(t, mass_own, ma):
        products(t, ma)
        if t > 0:
            note_change(t - 1)
        if t == 0:
            for k in range(early, nchunk):
                transpose(k)
            for cp in prow:
                cp.wait_recv()
            for part, tabs in enumerate([[row_send], [row_recv.at[d] for d in range(1, nc)]]):
                oh = row_onehot(tabs)
                ref = hot_far if part else hot_own
                ref[nr * slots :] = oh
                ref[0 : nr * slots] = dot(ohq[...], oh).astype(bf16)
            @pl.when(takes)
            def _():
                for cp in mate_rows:
                    cp.wait_recv()
                oh = row_onehot([rowp_recv.at[d] for d in range(nc)])
                hot_pair[...] = dot(ohcol[1], oh).astype(bf16)
                phi, plo = split(kinv_pair[...])
                kg_pair[...] = dot(ohcol[1], phi) + dot(ohcol[1], plo)

            khi, klo = split(kinv_ref[...])
            kg_ref[...] = dot(ohq[...], khi) + dot(ohq[...], klo)

        phi, plo = split(own_prod[...])
        last = t == ITERS - 1
        npick = 0 if last else nr * slots
        skip = nr * slots - npick
        near_sum = dot(hot_own[skip:], phi) + dot(hot_own[skip:], plo)

        up, down = spill_copies(t)

        @pl.when(l > 0)
        def _():
            up.wait_recv()

        @pl.when(l < nl - 1)
        def _():
            down.wait_recv()

        arrive = sp_recv[t, 0].astype(f32) + sp_recv[t, 1].astype(f32)
        mass = mass_own
        for cp in ma:
            cp.wait_recv()
        for i in range(len(peers)):
            mass = mass + ma_recv[t, i]
        flat = damping * (1.0 - coupling) * (jnp.sum(mass) / nodes) + (1.0 - damping)
        rest = damping * arrive + flat
        if not last:
            restg = damping * (dot(ohq[...], sp_recv[t, 0]) + dot(ohq[...], sp_recv[t, 1])) + flat

        if t == 0:
            rg_send[...] = restg[(nr - 1) * slots :]

            @pl.when(gives)
            def _():
                mate_rest.start()

        if not last:
            near_pick = gain * near_sum[0:npick] + restg
        near_walk = gain * near_sum[npick:] + rest
        for d in range(1, nc):
            for k, (at, n) in enumerate(cuts):
                remote(pr_send.at[t, pl.ds(at, n)], pr_recv.at[t, d, pl.ds(at, n)],
                       pr_ss.at[t, d, k], pr_rs.at[t, d, k],
                       l, r, lax.rem(c + d, nc)).wait_recv()
        far_sum = dot(hot_far[skip:], pr_recv[t, 1:nc].reshape((nc - 1) * slots, edge))
        if not last:
            pk = kg_ref[...] * (gain * far_sum[0:npick] + near_pick)
            for d in range(1, nr):
                pk_send[t + 1, d] = pk[d * slots : (d + 1) * slots].astype(bf16)
            pk_own[...] = pk[0:slots].astype(bf16).astype(f32)
            cps = pick_copies(t + 1)
            if t == 0:
                start_where([(cps[0], takes)])
                cps = cps[1:]
            for cp in cps:
                cp.start()
            sent.extend(cps)
        x = x_ref[...]
        updated = gain * far_sum[npick:] + near_walk
        x_ref[...] = updated
        diff[t] = fold(jnp.abs(updated - x))
        if last:
            note_change(t)
            return None
        send_spill(t + 1, updated, lax.rem(r, 2) == 1)
        return masses(t + 1)

    carry = masses(0)
    for t in range(ITERS):
        carry = step(t, *carry)

    rs_send[...] = chg[...]
    rs = []
    for dr, cc, dc in far_peers:
        i = dr * nc + dc - 1
        cp = remote(rs_send, rs_recv.at[i], rs_ss.at[i], rs_rs.at[i],
                    l, lax.rem(r + dr, nr), cc)
        cp.start()
        rs.append(cp)
    for h in range(halves):
        ranks_ref[pl.ds(h, blocks, stride=halves), :] = x_ref[:, h * 128 : (h + 1) * 128]
    for cp in px + pd + pc + prow + [e for q in pcs for e in q] + sent:
        cp.wait_send()

    @pl.when(gives)
    def _():
        for cp in mate_rows + mate_prods + [mate_rest]:
            cp.wait_send()

    @pl.when(takes)
    def _():
        pick_copies(1)[0].wait_send()

    ups = [spill_copies(t) for t in range(ITERS)]

    @pl.when(l < nl - 1)
    def _():
        for up, _ in ups:
            up.wait_send()

    @pl.when(l > 0)
    def _():
        for _, down in ups:
            down.wait_send()

    total = rs_send[...]
    for cp in rs:
        cp.wait_recv()
    for i in range(len(peers)):
        total = total + rs_recv[i]
    resid_ref[...] = total
    for cp in rs:
        cp.wait_send()


def scoped(sems, *args):
    pl.run_scoped(lambda *refs: kernel(*args, *refs), *sems)


def finish(ranks_in, resid_in, ranks_ref, resid_ref):
    ranks_ref[...] = ranks_in[...]
    resid_ref[...] = resid_in[:, 0:ITERS]


def local(block_values, block_rows, block_cols, block_count, dangling, start_ranks):
    span = start_ranks.shape[-1]
    nl, nr, nc = (lax.axis_size(a) for a in ("layer", "row", "col"))
    slots, edge = block_values.shape[3], block_values.shape[-1]
    blocks = span // edge
    nchunk = slots // PIECE
    nodes = nr * nc * span
    npeer = nr * nc - 1
    f32, bf16 = jnp.float32, jnp.bfloat16
    vm, dma = pltpu.VMEM, pltpu.SemaphoreType.DMA
    big = (blocks, edge)
    PT, ST = bf16, bf16
    scratch = [
        vm((slots, edge, edge), bf16), vm((slots, edge, edge), bf16), vm((span // 128, 128), jnp.int32), vm((span // 128, 128), f32),
        vm(big, f32), vm(big, f32), vm(big, f32),
        vm((slots, edge), f32), vm(big, f32), vm((slots, nc * slots), bf16), vm((nc, 1, 128), f32),
        vm((nc, slots, edge), PT), vm((slots, edge), f32), vm((slots, edge), f32),
        vm((nchunk, PIECE, edge), f32), vm((nr, slots, blocks), bf16),
        vm((slots, edge), f32), vm((ITERS, 8, 128), f32), vm((1, 128), f32),
        vm((slots, edge), f32), vm((ITERS, nr, slots, edge), bf16), vm((ITERS, nr, slots, edge), bf16),
        vm((nr * slots, edge), f32), vm((nr * slots + blocks, slots), bf16),
        vm((nr * slots + blocks, (nc - 1) * slots), bf16), vm((nr * slots, blocks), bf16),
        vm((nr, span // 128, 128), f32), vm((nr, span // 128, 128), jnp.int32),
        vm((1, 128), f32), vm((nr, 1, 128), f32), vm((nr, nchunk, PIECE, edge), f32),
        vm((1, 128), f32), vm((nc, 1, 128), f32),
        vm((nr,) + big, bf16),
        vm((ITERS, 1, 128), f32), vm((ITERS, npeer, 1, 128), f32),
        vm((ITERS, slots, edge), PT), vm((ITERS, nc, slots, edge), PT),
        vm((ITERS,) + big, ST), vm((ITERS, 2) + big, ST),
        vm((1, 128), f32), vm((npeer, 1, 128), f32),
        vm((1, slots), jnp.int32), vm((1, slots), jnp.int32), vm((1, 1), jnp.int32),
    ]
    sems = [
        dma((5,)), dma((nchunk,)),
        dma((nr,)), dma((nr,)), dma((nr,)), dma((nr,)), dma((nr,)), dma((nr,)),
        dma((nr, nchunk)), dma((nr, nchunk)), dma((nc,)), dma((nc,)),
        dma((ITERS, nr)), dma((ITERS, nr)), dma((ITERS, npeer)), dma((ITERS, npeer)),
        pltpu.SemaphoreType.REGULAR((2,)),
        dma((nc,)), dma((nc,)), dma((nc,)), dma((nc,)), dma((1,)), dma((1,)),
        dma((ITERS, nc, len(CUTS))), dma((ITERS, nc, len(CUTS))),
        dma((ITERS, 2)), dma((ITERS, 2)), dma((npeer,)), dma((npeer,)),
    ]
    hbm = pl.BlockSpec(memory_space=pltpu.HBM)
    vmem = pl.BlockSpec(memory_space=pltpu.VMEM)
    ranks, resid = pl.pallas_call(
        functools.partial(scoped, sems, nl, nr, nc, nodes),
        out_shape=(
            pltpu.VMEM((span // 128, 128), f32),
            pltpu.VMEM((1, 128), f32),
        ),
        in_specs=[hbm] * 6,
        out_specs=(vmem, vmem),
        scratch_shapes=scratch,
        compiler_params=pltpu.CompilerParams(collective_id=0, has_side_effects=True),
    )(
        block_values.reshape(slots, edge, edge),
        block_rows.reshape(1, slots),
        block_cols.reshape(1, slots),
        block_count.reshape(1, 1),
        dangling.reshape(span // 128, 128),
        start_ranks.reshape(span // 128, 128),
    )
    ranks, resid = pl.pallas_call(
        finish,
        out_shape=(
            jax.ShapeDtypeStruct((span // 128, 128), f32),
            jax.ShapeDtypeStruct((1, ITERS), f32),
        ),
        in_specs=[vmem, vmem],
        out_specs=(vmem, vmem),
        compiler_params=pltpu.CompilerParams(vmem_limit_bytes=4 * 1024 * 1024),
    )(ranks, resid)
    return ranks.reshape(1, 1, 1, span), resid.T


def solution(mesh):
    placed = (
        P("layer", "row", "col", None, None, None),
        P("layer", "row", "col", None),
        P("layer", "row", "col", None),
        P("layer", "row", "col"),
        P("layer", "row", "col", None),
        P("layer", "row", "col", None),
    )
    return jax.shard_map(
        local,
        mesh=mesh,
        in_specs=placed,
        out_specs=(P("layer", "row", "col", None), P(None, "layer")),
        check_vma=False,
    )
```

```python
import functools

import jax
import jax.numpy as jnp
from jax import lax
from jax.experimental import pallas as pl
from jax.experimental.pallas import tpu as pltpu
from jax.sharding import PartitionSpec as P

ITERS = 3
CHUNK = 16
PIECE = 8
CUTS = (16, 16)

damping = 0.85
coupling = 0.3


def fold(v):
    rows, lanes = v.shape
    acc = v[:, 0:128]
    for h in range(1, lanes // 128):
        acc = acc + v[:, h * 128 : (h + 1) * 128]
    return jnp.sum(acc.reshape(rows // 8, 8, 128), axis=0)


def split(v):
    hi = v.astype(jnp.bfloat16)
    lo = (v - hi.astype(jnp.float32)).astype(jnp.bfloat16)
    return hi, lo


def dot(a, b):
    return jnp.dot(a, b, preferred_element_type=jnp.float32)


def kernel(
    nl, nr, nc, nodes,
    values_hbm, rows_hbm, cols_hbm, count_hbm, dang_hbm, start_hbm,
    ranks_ref, resid_ref,
    values, vt, dang_in, start_in, x_ref, inv_ref, kinv_ref,
    kg_pair, kinv_pair, hot_pair, rowp_recv, pp_recv, rg_send, rg_recv,
    colsum, ohcol, own_prod, diff, chg,
    pk_own, pk_send, pk_recv, kg_ref, hot_own, hot_far, ohq,
    px_recv, pd_recv, col_send, col_recv, cs_recv, row_send, row_recv,
    sc_recv, ma_send, ma_recv,
    pr_send, pr_recv, sp_send, sp_recv, rs_send, rs_recv,
    rows_ref, cols_ref, count_ref,
    sem_in, sem_v,
    px_ss, px_rs, pd_ss, pd_rs, col_ss, col_rs, cs_ss, cs_rs, row_ss, row_rs, sc_ss, sc_rs, ma_ss, ma_rs,
    ready, rowp_ss, rowp_rs, pp_ss, pp_rs, rg_ss, rg_rs,
    pr_ss, pr_rs, sp_ss, sp_rs, rs_ss, rs_rs,
):
    l, r, c = (lax.axis_index(a) for a in ("layer", "row", "col"))
    slots, edge, _ = values.shape
    blocks = x_ref.shape[0]
    halves = edge // 128
    nchunk = slots // PIECE
    early = nchunk * 3 // 4
    gives = lax.rem(r, 2) == 0
    takes = lax.rem(r, 2) == 1
    mate = lax.rem(r + 1, nr)
    gain = damping * (1.0 - coupling)
    cuts = [(sum(CUTS[:i]), n) for i, n in enumerate(CUTS)]
    f32, bf16 = jnp.float32, jnp.bfloat16

    def remote(src, dst, ss, rs, ll, rr, cc):
        return pltpu.make_async_remote_copy(
            src_ref=src, dst_ref=dst, send_sem=ss, recv_sem=rs,
            device_id=(ll, rr, cc), device_id_type=pl.DeviceIdType.MESH,
        )

    in_d = pltpu.make_async_copy(dang_hbm, dang_in, sem_in.at[0])
    in_x = pltpu.make_async_copy(start_hbm, start_in, sem_in.at[1])
    vcopies = [
        pltpu.make_async_copy(
            values_hbm.at[pl.ds(k * PIECE, PIECE)], values.at[pl.ds(k * PIECE, PIECE)], sem_v.at[k]
        )
        for k in range(nchunk)
    ]
    small = [
        pltpu.make_async_copy(src, dst, sem_in.at[2 + i])
        for i, (src, dst) in enumerate(
            [(rows_hbm, rows_ref), (cols_hbm, cols_ref), (count_hbm, count_ref)])
    ]
    in_x.start()
    in_d.start()
    for cp in small:
        cp.start()
    for cp in vcopies:
        cp.start(priority=1)

    peers = [(dr, dc) for dr in range(nr) for dc in range(nc) if (dr, dc) != (0, 0)]
    barrier = pltpu.get_barrier_semaphore()
    def tell(sem, *to):
        pl.semaphore_signal(sem, inc=1, device_id=to, device_id_type=pl.DeviceIdType.MESH)

    for d in range(1, nr):
        tell(barrier, l, lax.rem(r + d, nr), c)
    for d in range(1, nc):
        @pl.when(c + d < nc)
        def _():
            for rr in range(nr):
                tell(barrier, l, rr, c + d)

    @pl.when(l < nl - 1)
    def _():
        tell(barrier, l + 1, r, c)

    for cp in small:
        cp.wait()
    live = lax.broadcasted_iota(jnp.int32, (1, slots), 1) < count_ref[...]
    rows = jnp.where(live, rows_ref[...], -1)
    cols = jnp.where(live, cols_ref[...], -1)
    pad = jnp.full((1, 128 - slots), -1, jnp.int32)
    row_send[...] = jnp.concatenate([rows, pad], axis=1).astype(f32)
    col_send[...] = jnp.concatenate([cols, pad], axis=1).astype(f32)

    eye = lax.broadcasted_iota(jnp.int32, (slots, slots), 0) == lax.broadcasted_iota(
        jnp.int32, (slots, slots), 1)

    def upright(tab):
        return jnp.sum(
            jnp.where(eye, jnp.broadcast_to(tab, (slots, slots)), 0.0), axis=1, keepdims=True)

    colv = upright(cols_ref[...].astype(f32))
    for d in range(nr):
        base = lax.rem(r - d + nr, nr) * blocks
        at = (lax.broadcasted_iota(jnp.int32, (slots, blocks), 1) + base).astype(f32)
        ohcol[d] = jnp.where(colv == at, 1.0, 0.0).astype(bf16)

    ones = jnp.ones((CHUNK, edge), bf16)
    rid = lax.broadcasted_iota(jnp.int32, (PIECE, edge), 0)

    def column_sum(k):
        vcopies[k].wait()
        acc = jnp.zeros((PIECE, edge), f32)
        for s in range(PIECE):
            acc = jnp.where(rid == s, dot(ones, values[k * PIECE + s])[0:PIECE], acc)
        colsum[k] = acc

    def transpose(k):
        for s in range(k * PIECE, (k + 1) * PIECE):
            vt[s] = values[s].T

    pl.semaphore_wait(barrier, nr - 1 + nr * c + (l > 0).astype(jnp.int32))
    for d in range(1, nc):
        @pl.when(c >= d)
        def _():
            for rr in range(nr):
                tell(ready.at[0], l, rr, c - d)

    @pl.when(l > 0)
    def _():
        tell(ready.at[1], l - 1, r, c)

    in_x.wait()
    in_d.wait()
    for h in range(halves):
        x_ref[:, h * 128 : (h + 1) * 128] = start_in[pl.ds(h, blocks, stride=halves), :]
    column_sum(0)

    order = []
    first, last = jnp.int32(0), jnp.int32(nc - 1)
    for _ in range(nc - 1):
        left = (c - first >= last - c).astype(jnp.int32)
        order.append(left * first + (1 - left) * last)
        first, last = first + left, last - (1 - left)
    far = [(cc, lax.rem(cc - c + nc, nc)) for cc in order]
    far_peers = [(dr, cc, d) for cc, d in far for dr in range(nr)]
    far_peers += [(dr, c, 0) for dr in range(1, nr)]
    sent = []

    px, pd, pc, pcs, prow = [], [], [], [], []
    for d in range(1, nr):
        rr = lax.rem(r + d, nr)
        px.append(remote(start_in, px_recv.at[d], px_ss.at[d], px_rs.at[d], l, rr, c))
        pd.append(remote(dang_in, pd_recv.at[d], pd_ss.at[d], pd_rs.at[d], l, rr, c))
        pc.append(remote(col_send, col_recv.at[d], col_ss.at[d], col_rs.at[d], l, rr, c))
        pcs.append([
            remote(colsum.at[k], cs_recv.at[d, k], cs_ss.at[d, k], cs_rs.at[d, k], l, rr, c)
            for k in range(nchunk)
        ])
    for cc, d in far:
        prow.append(remote(row_send, row_recv.at[d], row_ss.at[d], row_rs.at[d], l, r, cc))
    for cp in px + pd + pc + [q[0] for q in pcs]:
        cp.start()

    def start_where(pairs):
        for cp, cond in pairs:
            @pl.when(cond)
            def _():
                cp.start()

    start_where([(cp, cc < c) for cp, (cc, _) in zip(prow, far)])
    everyone = far + [(c, 0)]
    mate_rows = [
        remote(row_send, rowp_recv.at[d], rowp_ss.at[d], rowp_rs.at[d], l, mate, cc)
        for cc, d in everyone
    ]
    mate_prods = [
        remote(pr_send.at[0], pp_recv.at[d], pp_ss.at[d], pp_rs.at[d], l, mate, cc)
        for cc, d in everyone
    ]
    mate_rest = remote(rg_send, rg_recv, rg_ss.at[0], rg_rs.at[0], l, mate, c)
    start_where([(cp, gives & (cc <= c)) for cp, (cc, _) in zip(mate_rows, everyone)])

    def spill_copies(t):
        return (
            remote(sp_send.at[t], sp_recv.at[t, 0], sp_ss.at[t, 0], sp_rs.at[t, 0], l + 1, r, c),
            remote(sp_send.at[t], sp_recv.at[t, 1], sp_ss.at[t, 1], sp_rs.at[t, 1], l - 1, r, c),
        )

    spread = jnp.where((l == 0) | (l == nl - 1), 1.0, 0.5).astype(f32) * coupling

    def send_spill(t, x, when):
        if x is not None:
            sp_send[t] = (x * spread).astype(sp_send.dtype)
        up, down = spill_copies(t)

        @pl.when((l < nl - 1) & when)
        def _():
            up.start()

        @pl.when((l > 0) & when)
        def _():
            down.start()

    @pl.when(l == 0)
    def _():
        for t in range(ITERS):
            sp_recv[t, 0] = jnp.zeros((blocks, edge), sp_recv.dtype)

    @pl.when(l == nl - 1)
    def _():
        for t in range(ITERS):
            sp_recv[t, 1] = jnp.zeros((blocks, edge), sp_recv.dtype)

    for k in range(1, nchunk):
        column_sum(k)
        for q in pcs:
            q[k].start()
    for k in range(early):
        transpose(k)

    def hot(tab, rr):
        at = (lax.broadcasted_iota(jnp.int32, (blocks, slots), 0) + rr * blocks).astype(f32)
        return jnp.where(
            jnp.broadcast_to(tab[0:1, 0:slots], (blocks, slots)) == at, 1.0, 0.0).astype(bf16)

    def spread_sums(oh, sums):
        hi, lo = split(sums.reshape(slots, edge))
        return dot(oh, hi) + dot(oh, lo)

    def piece(buf, h):
        return buf[pl.ds(h, blocks, stride=halves), :]

    whose = [lax.rem(r - d + nr, nr) for d in range(nr)]
    near = [spread_sums(hot(col_send, rr), colsum[...]) for rr in whose]
    for cp in px + pd + pc:
        cp.wait_recv()
    peer_x = {d: jnp.concatenate([piece(px_recv.at[d], h) for h in range(halves)], axis=1)
              for d in range(1, nr)}
    keeps = {d: 1.0 - jnp.concatenate(
        [piece(pd_recv.at[d] if d else dang_in, h) for h in range(halves)], axis=1).astype(f32)
        for d in range(nr)}
    hots = [[hot(col_recv[e], rr) for e in range(1, nr)] for rr in whose]
    for e in range(nr):
        tab = colv if e == 0 else upright(col_recv[e][0:1, 0:slots])
        at = (lax.broadcasted_iota(jnp.int32, (slots, blocks), 1) + r * blocks).astype(f32)
        ohq[e * slots : (e + 1) * slots] = jnp.where(tab == at, 1.0, 0.0).astype(bf16)
    for q in pcs:
        for cp in q:
            cp.wait_recv()
    @pl.when(l < nl - 1)
    def _():
        pl.semaphore_wait(ready.at[1], 1)

    send_spill(0, x_ref[...], r >= 0)
    for d in range(nr):
        deg = near[d]
        for e in range(1, nr):
            deg = deg + spread_sums(hots[d][e - 1], cs_recv[e])
        inv = 1.0 / (keeps[d] * deg + 1.0)
        kinv = keeps[d] * inv
        if d == 0:
            inv_ref[...] = inv
            kinv_ref[...] = kinv
        else:
            sc_recv[d] = (peer_x[d] * kinv).astype(bf16)
            if d == 1:
                kinv_pair[...] = kinv

    def row_onehot(tabs):
        tab = jnp.concatenate([tab[0:1, 0:slots] for tab in tabs], axis=1)
        shape = (blocks, tab.shape[1])
        at = (lax.broadcasted_iota(jnp.int32, shape, 0) + c * blocks).astype(f32)
        return jnp.where(jnp.broadcast_to(tab, shape) == at, 1.0, 0.0).astype(bf16)

    def pick_copies(t):
        return [
            remote(pk_send.at[t, d], pk_recv.at[t, d], sc_ss.at[t, d], sc_rs.at[t, d],
                   l, lax.rem(r + d, nr), c)
            for d in range(1, nr)
        ]

    def picks(t):
        if t == 0:
            acc = dot(ohcol[0], (x_ref[...] * kinv_ref[...]).astype(bf16))
            for d in range(1, nr):
                acc = acc + dot(ohcol[d], sc_recv[d])
            return acc.astype(bf16)
        acc = pk_own[...]
        if t == 1:
            @pl.when(takes)
            def _():
                for cp in mate_prods + [mate_rest]:
                    cp.wait_recv()
                pw = dot(hot_pair[...], pp_recv[...].reshape(nc * slots, edge))
                pk_recv[1, 1] = (kg_pair[...] * (gain * pw + rg_recv[...])).astype(bf16)

        for d, cp in enumerate(pick_copies(t), 1):
            if t == 1 and d == 1:
                @pl.when(gives)
                def _():
                    cp.wait_recv()
            else:
                cp.wait_recv()
            acc = acc + pk_recv[t, d].astype(f32)
        return acc.astype(bf16)

    def products(t, ma):
        picked = picks(t)
        if t > 1:
            send_spill(t, None, gives)
        def piece_copy(k, cc, d):
            at, n = cuts[k]
            return remote(
                pr_send.at[t, pl.ds(at, n)], pr_recv.at[t, d, pl.ds(at, n)], pr_ss.at[t, d, k],
                pr_rs.at[t, d, k], l, r, cc)

        pr = []
        for k, (at, n) in enumerate(cuts):
            for at in range(at, at + n, PIECE):
                base = at // CHUNK * CHUNK
                lhs = picked[base : base + CHUNK]
                acc = jnp.zeros((PIECE, edge), f32)
                for s in range(PIECE):
                    if t == 0 and at >= early * PIECE:
                        res = lax.dot_general(
                            lhs, values[at + s], (((1,), (1,)), ((), ())),
                            preferred_element_type=f32)
                    else:
                        res = dot(lhs, vt[at + s])
                    acc = jnp.where(rid == s, res[at - base : at - base + PIECE], acc)
                own_prod[at : at + PIECE] = acc
                pr_send[t, at : at + PIECE] = acc.astype(pr_send.dtype)
            if t == 0 and k == 0:
                @pl.when(c < nc - 1)
                def _():
                    pl.semaphore_wait(ready.at[0], nr * (nc - 1 - c))

                start_where([(cp, cc > c) for cp, (cc, _) in zip(prow, far)])
                start_where([(cp, gives & (cc > c)) for cp, (cc, _) in zip(mate_rows, everyone)])
                start_where([(cp, cc > c) for cp, (_, cc, _) in zip(ma, far_peers)])
            pr += [piece_copy(k, *to) for to in (far[:-1] if k < len(cuts) - 1 else far)]
            for cp in pr[-len(far) + (k < len(cuts) - 1) :]:
                cp.start()
        for k in range(len(cuts) - 1):
            pr.append(piece_copy(k, *far[-1]))
            pr[-1].start()
        sent.extend(pr)
        if t == 0:
            @pl.when(gives)
            def _():
                for cp in mate_prods[-1:] + mate_prods[:-1]:
                    cp.start()


    def masses(t):
        mass_own = jnp.sum(fold(x_ref[...] * inv_ref[...]), axis=0, keepdims=True)
        ma_send[t] = mass_own
        ma = []
        for i, (dr, cc, dc) in enumerate(far_peers):
            slot = dr * nc + dc - 1
            ma.append(remote(ma_send.at[t], ma_recv.at[t, slot], ma_ss.at[t, slot],
                             ma_rs.at[t, slot], l, lax.rem(r + dr, nr), cc))
        if t == 0:
            start_where([(cp, cc <= c) for cp, (_, cc, _) in zip(ma, far_peers)])
        else:
            for cp in ma:
                cp.start()
        sent.extend(ma)
        return mass_own, ma

    def note_change(t):
        part = jnp.sum(diff[t], axis=0, keepdims=True)
        lane = lax.broadcasted_iota(jnp.int32, (1, 128), 1)
        old = chg[...] if t else jnp.zeros((1, 128), f32)
        chg[...] = jnp.where(lane == t, jnp.sum(part, axis=1, keepdims=True), old)

    def step(t, mass_own, ma):
        products(t, ma)
        if t > 0:
            note_change(t - 1)
        if t == 0:
            for k in range(early, nchunk):
                transpose(k)
            for cp in prow:
                cp.wait_recv()
            for part, tabs in enumerate([[row_send], [row_recv.at[d] for d in range(1, nc)]]):
                oh = row_onehot(tabs)
                ref = hot_far if part else hot_own
                ref[nr * slots :] = oh
                ref[0 : nr * slots] = dot(ohq[...], oh).astype(bf16)
            @pl.when(takes)
            def _():
                for cp in mate_rows:
                    cp.wait_recv()
                oh = row_onehot([rowp_recv.at[d] for d in range(nc)])
                hot_pair[...] = dot(ohcol[1], oh).astype(bf16)
                phi, plo = split(kinv_pair[...])
                kg_pair[...] = dot(ohcol[1], phi) + dot(ohcol[1], plo)

            khi, klo = split(kinv_ref[...])
            kg_ref[...] = dot(ohq[...], khi) + dot(ohq[...], klo)

        phi, plo = split(own_prod[...])
        last = t == ITERS - 1
        npick = 0 if last else nr * slots
        skip = nr * slots - npick
        near_sum = dot(hot_own[skip:], phi) + dot(hot_own[skip:], plo)

        up, down = spill_copies(t)

        @pl.when(l > 0)
        def _():
            up.wait_recv()

        @pl.when(l < nl - 1)
        def _():
            down.wait_recv()

        arrive = sp_recv[t, 0].astype(f32) + sp_recv[t, 1].astype(f32)
        mass = mass_own
        for cp in ma:
            cp.wait_recv()
        for i in range(len(peers)):
            mass = mass + ma_recv[t, i]
        flat = damping * (1.0 - coupling) * (jnp.sum(mass) / nodes) + (1.0 - damping)
        rest = damping * arrive + flat
        if not last:
            restg = damping * (dot(ohq[...], sp_recv[t, 0]) + dot(ohq[...], sp_recv[t, 1])) + flat

        if t == 0:
            rg_send[...] = restg[(nr - 1) * slots :]

            @pl.when(gives)
            def _():
                mate_rest.start()

        if not last:
            near_pick = gain * near_sum[0:npick] + restg
        near_walk = gain * near_sum[npick:] + rest
        for d in range(1, nc):
            for k, (at, n) in enumerate(cuts):
                remote(pr_send.at[t, pl.ds(at, n)], pr_recv.at[t, d, pl.ds(at, n)],
                       pr_ss.at[t, d, k], pr_rs.at[t, d, k],
                       l, r, lax.rem(c + d, nc)).wait_recv()
        far_sum = dot(hot_far[skip:], pr_recv[t, 1:nc].reshape((nc - 1) * slots, edge))
        if not last:
            pk = kg_ref[...] * (gain * far_sum[0:npick] + near_pick)
            for d in range(1, nr):
                pk_send[t + 1, d] = pk[d * slots : (d + 1) * slots].astype(bf16)
            pk_own[...] = pk[0:slots].astype(bf16).astype(f32)
            cps = pick_copies(t + 1)
            if t == 0:
                start_where([(cps[0], takes)])
                cps = cps[1:]
            for cp in cps:
                cp.start()
            sent.extend(cps)
        x = x_ref[...]
        updated = gain * far_sum[npick:] + near_walk
        x_ref[...] = updated
        diff[t] = fold(jnp.abs(updated - x))
        if last:
            note_change(t)
            return None
        out = masses(t + 1)
        send_spill(t + 1, updated, takes if t else r >= 0)
        return out

    carry = masses(0)
    for t in range(ITERS):
        carry = step(t, *carry)

    rs_send[...] = chg[...]
    rs = []
    for dr, cc, dc in far_peers:
        i = dr * nc + dc - 1
        cp = remote(rs_send, rs_recv.at[i], rs_ss.at[i], rs_rs.at[i],
                    l, lax.rem(r + dr, nr), cc)
        cp.start()
        rs.append(cp)
    for h in range(halves):
        ranks_ref[pl.ds(h, blocks, stride=halves), :] = x_ref[:, h * 128 : (h + 1) * 128]
    for cp in px + pd + pc + prow + [e for q in pcs for e in q] + sent:
        cp.wait_send()

    @pl.when(gives)
    def _():
        for cp in mate_rows + mate_prods + [mate_rest]:
            cp.wait_send()

    @pl.when(takes)
    def _():
        pick_copies(1)[0].wait_send()

    ups = [spill_copies(t) for t in range(ITERS)]

    @pl.when(l < nl - 1)
    def _():
        for up, _ in ups:
            up.wait_send()

    @pl.when(l > 0)
    def _():
        for _, down in ups:
            down.wait_send()

    total = rs_send[...]
    for cp in rs:
        cp.wait_recv()
    for i in range(len(peers)):
        total = total + rs_recv[i]
    resid_ref[...] = total
    for cp in rs:
        cp.wait_send()


def scoped(sems, *args):
    pl.run_scoped(lambda *refs: kernel(*args, *refs), *sems)


def finish(ranks_in, resid_in, ranks_ref, resid_ref):
    ranks_ref[...] = ranks_in[...]
    resid_ref[...] = resid_in[:, 0:ITERS]


def local(block_values, block_rows, block_cols, block_count, dangling, start_ranks):
    span = start_ranks.shape[-1]
    nl, nr, nc = (lax.axis_size(a) for a in ("layer", "row", "col"))
    slots, edge = block_values.shape[3], block_values.shape[-1]
    blocks = span // edge
    nchunk = slots // PIECE
    nodes = nr * nc * span
    npeer = nr * nc - 1
    f32, bf16 = jnp.float32, jnp.bfloat16
    vm, dma = pltpu.VMEM, pltpu.SemaphoreType.DMA
    big = (blocks, edge)
    PT, ST = bf16, bf16
    scratch = [
        vm((slots, edge, edge), bf16), vm((slots, edge, edge), bf16), vm((span // 128, 128), jnp.int32), vm((span // 128, 128), f32),
        vm(big, f32), vm(big, f32), vm(big, f32),
        vm((slots, edge), f32), vm(big, f32), vm((slots, nc * slots), bf16), vm((nc, 1, 128), f32),
        vm((nc, slots, edge), PT), vm((slots, edge), f32), vm((slots, edge), f32),
        vm((nchunk, PIECE, edge), f32), vm((nr, slots, blocks), bf16),
        vm((slots, edge), f32), vm((ITERS, 8, 128), f32), vm((1, 128), f32),
        vm((slots, edge), f32), vm((ITERS, nr, slots, edge), bf16), vm((ITERS, nr, slots, edge), bf16),
        vm((nr * slots, edge), f32), vm((nr * slots + blocks, slots), bf16),
        vm((nr * slots + blocks, (nc - 1) * slots), bf16), vm((nr * slots, blocks), bf16),
        vm((nr, span // 128, 128), f32), vm((nr, span // 128, 128), jnp.int32),
        vm((1, 128), f32), vm((nr, 1, 128), f32), vm((nr, nchunk, PIECE, edge), f32),
        vm((1, 128), f32), vm((nc, 1, 128), f32),
        vm((nr,) + big, bf16),
        vm((ITERS, 1, 128), f32), vm((ITERS, npeer, 1, 128), f32),
        vm((ITERS, slots, edge), PT), vm((ITERS, nc, slots, edge), PT),
        vm((ITERS,) + big, ST), vm((ITERS, 2) + big, ST),
        vm((1, 128), f32), vm((npeer, 1, 128), f32),
        vm((1, slots), jnp.int32), vm((1, slots), jnp.int32), vm((1, 1), jnp.int32),
    ]
    sems = [
        dma((5,)), dma((nchunk,)),
        dma((nr,)), dma((nr,)), dma((nr,)), dma((nr,)), dma((nr,)), dma((nr,)),
        dma((nr, nchunk)), dma((nr, nchunk)), dma((nc,)), dma((nc,)),
        dma((ITERS, nr)), dma((ITERS, nr)), dma((ITERS, npeer)), dma((ITERS, npeer)),
        pltpu.SemaphoreType.REGULAR((2,)),
        dma((nc,)), dma((nc,)), dma((nc,)), dma((nc,)), dma((1,)), dma((1,)),
        dma((ITERS, nc, len(CUTS))), dma((ITERS, nc, len(CUTS))),
        dma((ITERS, 2)), dma((ITERS, 2)), dma((npeer,)), dma((npeer,)),
    ]
    hbm = pl.BlockSpec(memory_space=pltpu.HBM)
    vmem = pl.BlockSpec(memory_space=pltpu.VMEM)
    ranks, resid = pl.pallas_call(
        functools.partial(scoped, sems, nl, nr, nc, nodes),
        out_shape=(
            pltpu.VMEM((span // 128, 128), f32),
            pltpu.VMEM((1, 128), f32),
        ),
        in_specs=[hbm] * 6,
        out_specs=(vmem, vmem),
        scratch_shapes=scratch,
        compiler_params=pltpu.CompilerParams(collective_id=0, has_side_effects=True),
    )(
        block_values.reshape(slots, edge, edge),
        block_rows.reshape(1, slots),
        block_cols.reshape(1, slots),
        block_count.reshape(1, 1),
        dangling.reshape(span // 128, 128),
        start_ranks.reshape(span // 128, 128),
    )
    ranks, resid = pl.pallas_call(
        finish,
        out_shape=(
            jax.ShapeDtypeStruct((span // 128, 128), f32),
            jax.ShapeDtypeStruct((1, ITERS), f32),
        ),
        in_specs=[vmem, vmem],
        out_specs=(vmem, vmem),
        compiler_params=pltpu.CompilerParams(vmem_limit_bytes=4 * 1024 * 1024),
    )(ranks, resid)
    return ranks.reshape(1, 1, 1, span), resid.T


def solution(mesh):
    placed = (
        P("layer", "row", "col", None, None, None),
        P("layer", "row", "col", None),
        P("layer", "row", "col", None),
        P("layer", "row", "col"),
        P("layer", "row", "col", None),
        P("layer", "row", "col", None),
    )
    return jax.shard_map(
        local,
        mesh=mesh,
        in_specs=placed,
        out_specs=(P("layer", "row", "col", None), P(None, "layer")),
        check_vma=False,
    )
```
